128 devices in a mesh: col: 16 (over x, y), cuts: 8 (over z, core).
Axes of the slice: x: 4, y: 4, z: 4, core: 2. Of those that a mesh axis runs over, the one named last changes fastest.
Arguments:
- layout: int32 [16, 16], P(None, 'col'), may hold values from 0 to 15
- assign: int32 [32, 16], P('cuts', 'col'), may hold values from 0 to 3
- edge: bfloat16 [16, 64, 128], replicated, may hold values from -3 to 3
- gate_left: bfloat16 [16, 16, 64, 128], P('col'), may hold values from -1.5 to 1.5
- gate_right: bfloat16 [16, 16, 64, 128], P('col'), may hold values from -1.5 to 1.5
- phase_angle: float32 [4, 64], replicated, may hold values from -3.140625 to 3.140625
- close: float32 [16, 64, 128], replicated, may hold values from -6 to 6
Outputs:
- slice_amplitude: float32 [32, 2], P('cuts')
- slice_log: float32 [32], P('cuts')
- total_amp: float32 [2], replicated
- top_log: float32 [], replicated
The draws below stay inside these ranges and needn't reach their ends.
All inputs are finite; a program needn't handle non-finite values. Where the reference program divides by a largest or mean magnitude, that divisor is 1e-20 or more.
Results may differ from the reference program's by a relative error of at most 0.0003.
Values sent between devices are 32-bit elements; how exact they have to be, the bound alone decides.
No kernel may reach another device: no remote copies, remote signals or barrier semaphores. Data moves between devices by JAX's collectives and lax.ppermute only.
A program may use at most 64 MiB of HBM per device.

```python
import math
import jax
import jax.numpy as jnp
from jax import lax

ROWS = 16
CHI = 64
NG = 16
QV = 4
COLS = 16
SLICES = 32


def plant(array, rng, low, top_value):
    index_at = [jax.random.randint(jax.random.fold_in(rng, axis), (), 0, length) for axis, length in enumerate(array.shape)]
    longest = array.shape.index(max(array.shape))
    neighbour = index_at[:longest] + [(index_at[longest] + 1) % array.shape[longest]] + index_at[longest + 1:]
    return array.at[tuple(index_at)].set(low).at[tuple(neighbour)].set(top_value)


def level_of(key, dims, shards, low, top_value):
    loudness, own = 1.0, jax.random.fold_in(key, 6)
    for axis_at, shards_of in shards:
        draws = jnp.exp(jax.random.uniform(jax.random.fold_in(own, axis_at), (shards_of,), jnp.float32, low / len(shards), top_value / len(shards)))
        loudness = loudness * jnp.repeat(draws, dims[axis_at] // shards_of).reshape([-1 if axis == axis_at else 1 for axis in range(len(dims))])
    return loudness


def scatter_about(rng, shape, scale, limit, pieces=(), dtype=jnp.bfloat16):
    entries = scale * jax.random.normal(rng, shape, jnp.float32)
    if pieces:
        entries = entries * level_of(rng, shape, pieces, -0.22, 0.18)
    return jnp.clip(entries, -limit, limit).astype(dtype)


def setup_inputs(seed: int = 0) -> dict:
    arg_keys = jax.random.split(jax.random.key(seed), 8)
    return {
        "layout": plant(jax.random.randint(arg_keys[0], (ROWS, COLS), 0, NG), jax.random.fold_in(arg_keys[0], 1), 0, NG - 1).astype(jnp.int32),
        "assign": plant(jax.random.randint(arg_keys[1], (SLICES, COLS), 0, QV), jax.random.fold_in(arg_keys[1], 1), 0, QV - 1).astype(jnp.int32),
        "edge": scatter_about(arg_keys[2], (ROWS, CHI, 2 * CHI), 0.5, 3.0),
        "gate_left": scatter_about(arg_keys[3], (COLS, NG, CHI, 2 * CHI), (CHI // 4) ** -0.5, 1.5, ((0, 16),)),
        "gate_right": scatter_about(arg_keys[4], (COLS, NG, CHI, 2 * CHI), (CHI // 4) ** -0.5, 1.5, ((0, 16),)),
        "phase_angle": jnp.clip(jax.random.uniform(arg_keys[5], (QV, CHI), jnp.float32, -3.140625, 3.140625), -3.140625, 3.140625),
        "close": scatter_about(arg_keys[6], (ROWS, CHI, 2 * CHI), 1.0, 6.0, (), jnp.float32),
    }


def sweep_column(board, scales, left_sel, right_sel, cosine, sine):
    width = board.shape[-2]
    below = jnp.concatenate([board[:, 1:], jnp.zeros_like(board[:, :1])], axis=1)
    mixed = board + 0.5 * below
    left_four = left_sel.astype(jnp.float32).reshape(left_sel.shape[0], width, 2, width)
    stacked = jnp.einsum('rpka,srab->srkpb', left_four, mixed, precision=lax.Precision.HIGHEST)
    former = stacked[:, :, 0]
    latter = stacked[:, :, 1]
    real_part = former[..., :width] - latter[..., width:]
    imag_part = former[..., width:] + latter[..., :width]
    right_wide = right_sel.astype(jnp.float32)
    from_real = jnp.einsum('srab,rbq->sraq', real_part, right_wide, precision=lax.Precision.HIGHEST)
    from_imag = jnp.einsum('srab,rbq->sraq', imag_part, right_wide, precision=lax.Precision.HIGHEST)
    out_real = from_real[..., :width] - from_imag[..., width:]
    out_imag = from_real[..., width:] + from_imag[..., :width]
    cos_rows = cosine[:, None, None, :]
    sin_rows = sine[:, None, None, :]
    turned_real = out_real * cos_rows - out_imag * sin_rows
    turned_imag = out_real * sin_rows + out_imag * cos_rows
    peaks = jnp.maximum(lax.optimization_barrier(jnp.max(jnp.abs(turned_real), axis=(1, 2, 3))), lax.optimization_barrier(jnp.max(jnp.abs(turned_imag), axis=(1, 2, 3))))
    peaks = jnp.maximum(peaks, 1.0)
    board = jnp.concatenate([turned_real, turned_imag], -1) / peaks[:, None, None, None]
    return (board, scales + jnp.log(peaks))

def amplitude(board, close):
    width = close.shape[-1] // 2
    b_real = board[..., :width]
    b_imag = board[..., width:]
    c_real = close[..., :width]
    c_imag = close[..., width:]
    factor = 1.0 / math.sqrt(close.shape[0] * width * width)
    amp_real = lax.optimization_barrier(jnp.sum(b_real * c_real - b_imag * c_imag, axis=(1, 2, 3))) * factor
    amp_imag = lax.optimization_barrier(jnp.sum(b_real * c_imag + b_imag * c_real, axis=(1, 2, 3))) * factor
    return jnp.stack([amp_real, amp_imag], -1)

def reference(layout, assign, edge, gate_left, gate_right, phase_angle, close):
    count = assign.shape[0]
    board = jnp.broadcast_to(edge.astype(jnp.float32)[None], (count,) + edge.shape)
    scales = jnp.zeros((count,), jnp.float32)
    cos_table = jnp.cos(phase_angle)
    sin_table = jnp.sin(phase_angle)

    def advance(carry, inputs):
        board, scales = carry
        left_col, right_col, kinds, values = inputs
        left_sel = left_col[kinds.astype(jnp.int32)]
        right_sel = right_col[kinds.astype(jnp.int32)]
        cosine = cos_table[values.astype(jnp.int32)]
        sine = sin_table[values.astype(jnp.int32)]
        return (sweep_column(board, scales, left_sel, right_sel, cosine, sine), None)
    (board, scales), unused = lax.scan(advance, (board, scales), (gate_left, gate_right, layout.T, assign.T))
    amps = amplitude(board, close)
    top_log = jnp.max(scales)
    total_amp = lax.optimization_barrier(jnp.sum(amps * jnp.exp(scales - top_log)[:, None], axis=0))
    return (amps, scales, total_amp, top_log)
```

```python
import math

import jax
import jax.numpy as jnp
from jax import lax
from jax.experimental import pallas as pl
from jax.experimental.pallas import tpu as pltpu
from jax.sharding import Mesh
from jax.sharding import PartitionSpec as P

AXES = ("s", "xp", "q", "yp", "z", "c")
GRID = ("s", "xp", "q", "yp")
NC = 8
NR = 8
W = 64
BLOCK = 4 * 2 * W + 8
BOARD = NR * W + 8
HALO = NC * W + 16
F32 = jnp.float32
BF16 = jnp.bfloat16


def vmem():
    return pl.BlockSpec(memory_space=pltpu.VMEM)


def smem():
    return pl.BlockSpec(memory_space=pltpu.SMEM)


def sign_row():
    lane = lax.broadcasted_iota(jnp.int32, (1, 2 * W), 1)
    return jnp.where(lane < W, -1.0, 1.0).astype(F32)


def times_i(x, sign):
    return pltpu.roll(x, W, 1) * sign


def pack_kernel(layout, assign, left, right, out):
    core = lax.axis_index("c")
    for t in range(4):
        row = jnp.full((1, 2 * W), assign[t, 0].astype(F32), F32)
        for dest in range(8):
            out[dest, pl.ds(8 * W + t, 1), :] = row
    for dest in range(8):
        out[dest, pl.ds(8 * W + 4, 4), :] = jnp.zeros((4, 2 * W), F32)
    for half in range(2):
        for k in range(4):
            kind = layout[(1 - half) * NR + 4 * core + k, 0]
            a = left[0, kind].astype(F32)
            b = right[0, kind].astype(F32)
            for xp in range(2):
                for yp in range(2):
                    dest = 4 * xp + 2 * half + yp
                    out[dest, pl.ds(2 * W * k, W), :] = a
                    out[dest, pl.ds(2 * W * k + W, W), :] = b


def unpack_gates(mine, other, lefts, rights, core, sign):
    def place(j, unused):
        for source, part in ((mine, core), (other, 1 - core)):
            for k in range(4):
                row = 4 * part + k
                lefts[j, row] = source[j, pl.ds(2 * W * k, W), :].astype(BF16)
                r = source[j, pl.ds(2 * W * k + W, W), :]
                rights[j, row, pl.ds(0, W), :] = r.astype(BF16)
                rights[j, row, pl.ds(W, W), :] = times_i(r, sign).astype(BF16)
        return unused

    lax.fori_loop(0, NC, place, 0)


def halves(x):
    high = x.astype(BF16)
    return high, (x - high.astype(F32)).astype(BF16)


def sweep(state, lefts, rights, mine, cosine, sine, halo_in, halo_out, peaks, own, start, sign):
    p0, mix0, rho0 = start

    def column(j, carry):
        p, rho_mix, rho = carry
        value = mine[j, pl.ds(8 * W + own, 1), :]
        cos_row = jnp.zeros((1, 2 * W), F32)
        sin_row = jnp.zeros((1, 2 * W), F32)
        for v in range(4):
            hit = value == float(v)
            cos_row = jnp.where(hit, cosine[pl.ds(v, 1), :], cos_row)
            sin_row = jnp.where(hit, sine[pl.ds(v, 1), :], sin_row)
        scale = 1.0 / p
        cos_row = cos_row * scale
        sin_row = sin_row * scale
        boards = [state[k] for k in range(NR)]
        halo_out[pl.ds(pl.multiple_of(j * W, W), W), :] = boards[0]
        if halo_in is None:
            below = None
        else:
            below = halo_in[pl.ds(pl.multiple_of(j * W, W), W), :] * rho_mix
        top = jnp.zeros((8, 2 * W), F32)
        for k in range(NR):
            after = boards[k + 1] if k + 1 < NR else below
            mixed = boards[k] if after is None else boards[k] + 0.5 * after
            turn = times_i(mixed, sign)
            mh, ml = halves(mixed)
            th, tl = halves(turn)
            gate = lefts[j, k]
            middle = jnp.dot(
                jnp.concatenate([gate, gate], 1),
                jnp.concatenate([mh, th, ml, tl], 0),
                preferred_element_type=F32,
            )
            dh, dl = halves(middle)
            right = rights[j, k]
            out = jnp.dot(
                jnp.concatenate([dh, dl], 1),
                jnp.concatenate([right, right], 0),
                preferred_element_type=F32,
            )
            out = out * cos_row + pltpu.roll(out, W, 1) * sin_row
            state[k] = out
            for g in range(8):
                top = jnp.maximum(top, jnp.abs(out[8 * g : 8 * g + 8]))
        own_top = jnp.broadcast_to(jnp.max(top, keepdims=True), (1, 2 * W))
        halo_out[pl.ds(NC * W + j, 1), :] = own_top
        if halo_in is None:
            other_top = jnp.zeros((1, 2 * W), F32)
        else:
            other_top = halo_in[pl.ds(NC * W + j, 1), :]
        p_new = jnp.maximum(jnp.maximum(own_top, other_top * rho), 1.0)
        peaks[pl.ds(j, 1), :] = p_new
        return (p_new, rho, rho * jnp.maximum(other_top, 1.0) / p_new)

    return lax.fori_loop(0, NC, column, (p0, mix0, rho0))


def close_sums(state, close, base, sign):
    real = jnp.zeros((8, 2 * W), F32)
    imag = jnp.zeros((8, 2 * W), F32)
    for k in range(NR):
        c = close[base + k]
        b = state[k]
        d = pltpu.roll(c, W, 1)
        for g in range(8):
            part = slice(8 * g, 8 * g + 8)
            real = real - b[part] * c[part] * sign
            imag = imag + b[part] * d[part]
    return jnp.sum(real, keepdims=True), jnp.sum(imag, keepdims=True)


def write_messages(state, board_out, halo_out, peaks, ell, end, sums):
    p, rho_mix, rho = end
    for k in range(NR):
        board_out[pl.ds(k * W, W), :] = state[k]
    board_out[pl.ds(NR * W, 1), :] = p
    board_out[pl.ds(NR * W + 1, 1), :] = rho_mix
    board_out[pl.ds(NR * W + 2, 1), :] = rho
    board_out[pl.ds(NR * W + 3, 1), :] = ell + jnp.sum(jnp.log(peaks[...]), axis=0, keepdims=True)
    board_out[pl.ds(NR * W + 4, 4), :] = jnp.zeros((4, 2 * W), F32)
    halo_out[pl.ds(NC * W + 8, 8), :] = jnp.zeros((8, 2 * W), F32)
    if sums is not None:
        halo_out[pl.ds(NC * W + 8, 1), :] = jnp.broadcast_to(sums[0], (1, 2 * W))
        halo_out[pl.ds(NC * W + 9, 1), :] = jnp.broadcast_to(sums[1], (1, 2 * W))


def places():
    s, q = lax.axis_index("s"), lax.axis_index("q")
    i = jnp.where(s == 0, lax.axis_index("xp"), 1 - lax.axis_index("xp"))
    j = jnp.where(q == 0, lax.axis_index("yp"), 1 - lax.axis_index("yp"))
    return s, q, 2 * i + j, (1 - q) * NR


def first_kernel(mine, other, edge, cosine, sine, lefts, rights, board_out, halo_out, state, peaks):
    s, q, own, base = places()
    sign = sign_row()
    one = jnp.ones((1, 2 * W), F32)
    unpack_gates(mine, other, lefts, rights, lax.axis_index("c"), sign)
    for k in range(NR):
        state[k] = edge[base + k].astype(F32)
    end = sweep(
        state, lefts, rights, mine, cosine, sine, None, halo_out, peaks, own, (one, one, one), sign
    )
    write_messages(state, board_out, halo_out, peaks, 0.0 * one, end, None)


def load_state(state, edge, board_in, base, s):
    one = jnp.ones((1, 2 * W), F32)
    first = s == 0
    for k in range(NR):
        state[k] = jnp.where(first, edge[base + k].astype(F32), board_in[pl.ds(k * W, W), :])
    row = lambda n: board_in[pl.ds(NR * W + n, 1), :]
    p = jnp.maximum(jnp.where(first, one, row(0)), 1.0)
    rho_mix = jnp.where(first, one, row(1))
    rho = jnp.where(first, one, row(2))
    ell = jnp.where(first, 0.0 * one, row(3))
    return (p, rho_mix, rho), ell


def second_kernel(mine, edge, cosine, sine, lefts, rights, close, board_in, halo_in, board_out, halo_out, state, peaks):
    s, q, own, base = places()
    sign = sign_row()
    start, ell = load_state(state, edge, board_in, base, s)
    end = sweep(
        state, lefts, rights, mine, cosine, sine, halo_in, halo_out, peaks, own, start, sign
    )
    write_messages(
        state, board_out, halo_out, peaks, ell, end, close_sums(state, close, base, sign)
    )


def third_kernel(mine, edge, cosine, sine, lefts, rights, close, board_in, halo_in, out, state, peaks, halo_out):
    s, q, own, base = places()
    sign = sign_row()
    start, ell = load_state(state, edge, board_in, base, s)
    p, rho_mix, rho = sweep(
        state, lefts, rights, mine, cosine, sine, halo_in, halo_out, peaks, own, start, sign
    )
    ell = ell + jnp.sum(jnp.log(peaks[...]), axis=0, keepdims=True)
    real, imag = close_sums(state, close, base, sign)
    factor = 1.0 / math.sqrt(2 * NR * W * W)
    real = (real + rho_mix * halo_in[pl.ds(NC * W + 8, 1), :]) / p * factor
    imag = (imag + rho_mix * halo_in[pl.ds(NC * W + 9, 1), :]) / p * factor
    index = 4 * (2 * lax.axis_index("z") + lax.axis_index("c")) + own
    lane = lax.broadcasted_iota(jnp.int32, (1, 2 * W), 1)
    index = jnp.where(jnp.logical_and(s == 1, q == 1), index, -1)
    hit = lane == index
    zero = jnp.zeros((1, 2 * W), F32)
    out[pl.ds(0, 1), :] = jnp.where(hit, real, zero)
    out[pl.ds(1, 1), :] = jnp.where(hit, imag, zero)
    out[pl.ds(2, 1), :] = jnp.where(hit, ell, zero)
    out[pl.ds(3, 5), :] = jnp.zeros((5, 2 * W), F32)


def call(kernel, outs, scratch, args, specs=None):
    return pl.pallas_call(
        kernel,
        out_shape=outs,
        in_specs=specs or [vmem()] * len(args),
        out_specs=jax.tree.map(lambda _: vmem(), outs),
        scratch_shapes=scratch,
        compiler_params=pltpu.CompilerParams(vmem_limit_bytes=48 * 2**20),
    )(*args)


def shape(*dims, dtype=F32):
    return jax.ShapeDtypeStruct(dims, dtype)


def chip(s, xp, q, yp):
    return 8 * s + 4 * xp + 2 * q + yp


def along_columns(value, q):
    pairs = [(chip(0, xp, q, yp), chip(1, 1 - xp, q, yp)) for xp in range(2) for yp in range(2)]
    return lax.ppermute(value, GRID, pairs)


def along_rows(value, s):
    pairs = [(chip(s, xp, 0, yp), chip(s, xp, 1, 1 - yp)) for xp in range(2) for yp in range(2)]
    return lax.ppermute(value, GRID, pairs)


def around(value, axis):
    length = lax.axis_size(axis)
    total = value
    for by in range(1, length):
        pairs = [(i, (i + by) % length) for i in range(length)]
        total = total + lax.ppermute(value, axis, pairs)
    return total


def body(layout, assign, edge, gate_left, gate_right, phase_angle, close):
    cosine, sine = jnp.cos(phase_angle), jnp.sin(phase_angle)
    cosine = jnp.concatenate([cosine, cosine], -1)
    sine = jnp.concatenate([-sine, sine], -1)
    packed = call(
        pack_kernel,
        shape(8, BLOCK, 2 * W),
        [],
        (layout, assign, gate_left, gate_right),
        [smem(), smem(), vmem(), vmem()],
    )
    mine = lax.all_to_all(packed, ("xp", "q", "yp"), 0, 0, tiled=True)
    other = lax.ppermute(mine, "c", [(0, 1), (1, 0)])
    state = pltpu.VMEM((NR, W, 2 * W), F32)
    peaks = pltpu.VMEM((NC, 2 * W), F32)
    lefts, rights, board, halo = call(
        first_kernel,
        (
            shape(NC, NR, W, 2 * W, dtype=BF16),
            shape(NC, NR, 2 * W, 2 * W, dtype=BF16),
            shape(BOARD, 2 * W),
            shape(HALO, 2 * W),
        ),
        [state, peaks],
        (mine, other, edge, cosine, sine),
    )
    board, halo = along_columns(board, 0), along_rows(halo, 0)
    board, halo = call(
        second_kernel,
        (shape(BOARD, 2 * W), shape(HALO, 2 * W)),
        [state, peaks],
        (mine, edge, cosine, sine, lefts, rights, close, board, halo),
    )
    board, halo = along_columns(board, 1), along_rows(halo, 1)
    found = call(
        third_kernel,
        shape(8, 2 * W),
        [state, peaks, pltpu.VMEM((HALO, 2 * W), F32)],
        (mine, edge, cosine, sine, lefts, rights, close, board, halo),
    )
    for axis in ("c", ("s", "xp"), ("q", "yp"), "z"):
        found = around(found, axis)
    logs = found[2, :32]
    top_log = jnp.max(logs)
    total_amp = jnp.sum(found[:2, :32] * jnp.exp(logs - top_log)[None], axis=1)
    at = 4 * (2 * lax.axis_index("z") + lax.axis_index("c"))
    here = lax.dynamic_slice_in_dim(found, at, 4, 1)
    return (here[:2].T, here[2], total_amp, top_log)


def solution(mesh):
    split = Mesh(mesh.devices.reshape(2, 2, 2, 2, 4, 2), AXES)
    placed = (
        P(None, GRID),
        P(("z", "c"), GRID),
        P(),
        P(GRID, None, None, None),
        P(GRID, None, None, None),
        P(),
        P(),
    )
    return jax.shard_map(
        body,
        mesh=split,
        in_specs=placed,
        out_specs=(P(("z", "c"), None), P(("z", "c")), P(), P()),
        check_vma=False,
    )
```

```python
import math

import jax
import jax.numpy as jnp
from jax import lax
from jax.experimental import pallas as pl
from jax.experimental.pallas import tpu as pltpu
from jax.sharding import Mesh
from jax.sharding import PartitionSpec as P

AXES = ("s", "xp", "q", "yp", "z", "c")
GRID = ("s", "xp", "q", "yp")
NC = 8
NR = 8
W = 64
BLOCK = 4 * 2 * W + 8
BOARD = NR * W + 8
HALO = NC * W + 16
F32 = jnp.float32
BF16 = jnp.bfloat16


def vmem():
    return pl.BlockSpec(memory_space=pltpu.VMEM)


def sign_row():
    lane = lax.broadcasted_iota(jnp.int32, (1, 2 * W), 1)
    return jnp.where(lane < W, -1.0, 1.0).astype(F32)


def times_i(x, sign):
    return pltpu.roll(x, W, 1) * sign


def pack_kernel(layout_hbm, assign_hbm, left, right, out, layout, assign, raw, sems):
    core = lax.axis_index("c")
    small = [
        pltpu.make_async_copy(layout_hbm, layout, sems.at[16]),
        pltpu.make_async_copy(assign_hbm, assign, sems.at[17]),
    ]
    for copy in small:
        copy.start()
    for copy in small:
        copy.wait()
    copies = []
    for half in range(2):
        for k in range(4):
            kind = layout[0, (1 - half) * NR + 4 * core + k]
            for side, table in ((0, left), (1, right)):
                n = 8 * half + 2 * k + side
                copies.append(pltpu.make_async_copy(table.at[0, kind], raw.at[n], sems.at[n]))
                copies[-1].start()
    for t in range(4):
        row = jnp.full((1, 2 * W), assign[0, t].astype(F32), F32)
        for dest in range(8):
            out[dest, pl.ds(8 * W + t, 1), :] = row
    for dest in range(8):
        out[dest, pl.ds(8 * W + 4, 4), :] = jnp.zeros((4, 2 * W), F32)
    for n in range(16):
        copies[n].wait()
        x = raw[n].astype(F32)
        half, row = n // 8, n % 8
        for xp in range(2):
            for yp in range(2):
                out[4 * xp + 2 * half + yp, pl.ds(W * row, W), :] = x


def unpack(source, part, lefts, rights, sign):
    def place(j, unused):
        for k in range(4):
            row = 4 * part + k
            lefts[j, row] = source[j, pl.ds(2 * W * k, W), :].astype(BF16)
            r = source[j, pl.ds(2 * W * k + W, W), :]
            rights[j, row, pl.ds(0, W), :] = r.astype(BF16)
            rights[j, row, pl.ds(W, W), :] = times_i(r, sign).astype(BF16)
        return unused

    lax.fori_loop(0, NC, place, 0)


def unpack_kernel(mine, cosine, sine, lefts, rights, phases):
    s, q, own, base = places()
    unpack(mine, lax.axis_index("c"), lefts, rights, sign_row())
    for j in range(NC):
        value = mine[j, pl.ds(8 * W + own, 1), :]
        for n, table in ((0, cosine), (NC, sine)):
            row = jnp.zeros((1, 2 * W), F32)
            for v in range(4):
                row = jnp.where(value == float(v), table[pl.ds(v, 1), :], row)
            phases[pl.ds(n + j, 1), :] = row


def halves(x):
    high = x.astype(BF16)
    return high, (x - high.astype(F32)).astype(BF16)


def sweep(state, lefts, rights, phases, halo_in, halo_out, peaks, start, sign):
    def column(j, carry):
        p, rho_mix, rho = carry
        scale = 1.0 / p
        cos_row = phases[pl.ds(j, 1), :] * scale
        sin_row = phases[pl.ds(NC + j, 1), :] * scale
        boards = [state[k] for k in range(NR)]
        halo_out[pl.ds(j * W, W), :] = boards[0]
        if halo_in is None:
            below = None
        else:
            below = halo_in[pl.ds(j * W, W), :] * rho_mix
        top = jnp.zeros((8, 2 * W), F32)
        for k in range(NR):
            after = boards[k + 1] if k + 1 < NR else below
            mixed = boards[k] if after is None else boards[k] + 0.5 * after
            turn = times_i(mixed, sign)
            mh, ml = halves(mixed)
            th, tl = halves(turn)
            both = jnp.dot(
                lefts[j, k],
                jnp.concatenate([jnp.concatenate([mh, th], 0), jnp.concatenate([ml, tl], 0)], 1),
                preferred_element_type=F32,
            )
            middle = both[:, : 2 * W] + both[:, 2 * W :]
            dh, dl = halves(middle)
            two = jnp.dot(
                jnp.concatenate([dh, dl], 0), rights[j, k], preferred_element_type=F32
            )
            out = two[:W] + two[W:]
            out = out * cos_row + pltpu.roll(out, W, 1) * sin_row
            state[k] = out
            for g in range(8):
                top = jnp.maximum(top, jnp.abs(out[8 * g : 8 * g + 8]))
        own_top = jnp.broadcast_to(jnp.max(top, keepdims=True), (1, 2 * W))
        halo_out[pl.ds(NC * W + j, 1), :] = own_top
        if halo_in is None:
            other_top = jnp.zeros((1, 2 * W), F32)
        else:
            other_top = halo_in[pl.ds(NC * W + j, 1), :]
        p_new = jnp.maximum(jnp.maximum(own_top, other_top * rho), 1.0)
        peaks[pl.ds(j, 1), :] = p_new
        return (p_new, rho, rho * jnp.maximum(other_top, 1.0) / p_new)

    carry = start
    for j in range(NC):
        carry = column(j, carry)
    return carry


def close_sums(state, close, base, sign):
    real = jnp.zeros((8, 2 * W), F32)
    imag = jnp.zeros((8, 2 * W), F32)
    for k in range(NR):
        c = close[base + k]
        b = state[k]
        d = pltpu.roll(c, W, 1)
        for g in range(8):
            part = slice(8 * g, 8 * g + 8)
            real = real - b[part] * c[part] * sign
            imag = imag + b[part] * d[part]
    return jnp.sum(real, keepdims=True), jnp.sum(imag, keepdims=True)


def write_messages(state, board_out, halo_out, peaks, ell, end, sums):
    p, rho_mix, rho = end
    for k in range(NR):
        board_out[pl.ds(k * W, W), :] = state[k]
    board_out[pl.ds(NR * W, 1), :] = p
    board_out[pl.ds(NR * W + 1, 1), :] = rho_mix
    board_out[pl.ds(NR * W + 2, 1), :] = rho
    board_out[pl.ds(NR * W + 3, 1), :] = ell + jnp.sum(jnp.log(peaks[...]), axis=0, keepdims=True)
    board_out[pl.ds(NR * W + 4, 4), :] = jnp.zeros((4, 2 * W), F32)
    halo_out[pl.ds(NC * W + 8, 8), :] = jnp.zeros((8, 2 * W), F32)
    if sums is not None:
        halo_out[pl.ds(NC * W + 8, 1), :] = jnp.broadcast_to(sums[0], (1, 2 * W))
        halo_out[pl.ds(NC * W + 9, 1), :] = jnp.broadcast_to(sums[1], (1, 2 * W))


def places():
    s, q = lax.axis_index("s"), lax.axis_index("q")
    i = jnp.where(s == 0, lax.axis_index("xp"), 1 - lax.axis_index("xp"))
    j = jnp.where(q == 0, lax.axis_index("yp"), 1 - lax.axis_index("yp"))
    return s, q, 2 * i + j, (1 - q) * NR


def first_kernel(other, lefts_in, rights_in, phases, edge, lefts, rights, board_out, halo_out, state, peaks):
    s, q, own, base = places()
    sign = sign_row()
    one = jnp.ones((1, 2 * W), F32)
    unpack(other, 1 - lax.axis_index("c"), lefts, rights, sign)
    for k in range(NR):
        state[k] = edge[base + k].astype(F32)
    end = sweep(state, lefts, rights, phases, None, halo_out, peaks, (one, one, one), sign)
    write_messages(state, board_out, halo_out, peaks, 0.0 * one, end, None)


def load_state(state, edge, board_in, base, s):
    one = jnp.ones((1, 2 * W), F32)
    first = s == 0
    for k in range(NR):
        state[k] = jnp.where(first, edge[base + k].astype(F32), board_in[pl.ds(k * W, W), :])
    row = lambda n: board_in[pl.ds(NR * W + n, 1), :]
    p = jnp.maximum(jnp.where(first, one, row(0)), 1.0)
    rho_mix = jnp.where(first, one, row(1))
    rho = jnp.where(first, one, row(2))
    ell = jnp.where(first, 0.0 * one, row(3))
    return (p, rho_mix, rho), ell


def second_kernel(phases, edge, lefts, rights, close, board_in, halo_in, board_out, halo_out, state, peaks):
    s, q, own, base = places()
    sign = sign_row()
    start, ell = load_state(state, edge, board_in, base, s)
    end = sweep(state, lefts, rights, phases, halo_in, halo_out, peaks, start, sign)
    write_messages(
        state, board_out, halo_out, peaks, ell, end, close_sums(state, close, base, sign)
    )


def third_kernel(phases, edge, lefts, rights, close, board_in, halo_in, out, state, peaks, halo_out):
    s, q, own, base = places()
    sign = sign_row()
    start, ell = load_state(state, edge, board_in, base, s)
    p, rho_mix, rho = sweep(state, lefts, rights, phases, halo_in, halo_out, peaks, start, sign)
    ell = ell + jnp.sum(jnp.log(peaks[...]), axis=0, keepdims=True)
    real, imag = close_sums(state, close, base, sign)
    factor = 1.0 / math.sqrt(2 * NR * W * W)
    real = (real + rho_mix * halo_in[pl.ds(NC * W + 8, 1), :]) / p * factor
    imag = (imag + rho_mix * halo_in[pl.ds(NC * W + 9, 1), :]) / p * factor
    index = 4 * (2 * lax.axis_index("z") + lax.axis_index("c")) + own
    lane = lax.broadcasted_iota(jnp.int32, (1, 2 * W), 1)
    index = jnp.where(jnp.logical_and(s == 1, q == 1), index, -1)
    hit = lane == index
    zero = jnp.zeros((1, 2 * W), F32)
    out[pl.ds(0, 1), :] = jnp.where(hit, real, zero)
    out[pl.ds(1, 1), :] = jnp.where(hit, imag, zero)
    out[pl.ds(2, 1), :] = jnp.where(hit, ell, zero)
    out[pl.ds(3, 5), :] = jnp.zeros((5, 2 * W), F32)


def finish_kernel(a, b, c, d, amps, logs, total, top):
    found = a[...] + b[...] + c[...] + d[...]
    ell = found[2:3]
    high = jnp.max(ell, axis=1, keepdims=True)
    weighted = found[0:2] * jnp.exp(ell - high)
    top[...] = high
    sums = jnp.sum(weighted, axis=1, keepdims=True)
    total[...] = jnp.concatenate([sums[0:1], sums[1:2]], 1)
    at = 4 * (2 * lax.axis_index("z") + lax.axis_index("c"))
    here = pltpu.roll(found, jnp.where(at == 0, 0, 2 * W - at), 1)
    amps[...] = here[0:2, 0:4]
    logs[...] = here[2:3, 0:4]


def call(kernel, outs, scratch, args, specs=None, aliases=None):
    return pl.pallas_call(
        kernel,
        out_shape=outs,
        in_specs=specs or [vmem()] * len(args),
        out_specs=jax.tree.map(lambda _: vmem(), outs),
        scratch_shapes=scratch,
        input_output_aliases=aliases or {},
        compiler_params=pltpu.CompilerParams(vmem_limit_bytes=20 * 2**20),
    )(*args)


def shape(*dims, dtype=F32):
    return jax.ShapeDtypeStruct(dims, dtype)


def chip(s, xp, q, yp):
    return 8 * s + 4 * xp + 2 * q + yp


def along_columns(value, q):
    pairs = [(chip(0, xp, q, yp), chip(1, 1 - xp, q, yp)) for xp in range(2) for yp in range(2)]
    return lax.ppermute(value, GRID, pairs)


def along_rows(value, s):
    pairs = [(chip(s, xp, 0, yp), chip(s, xp, 1, 1 - yp)) for xp in range(2) for yp in range(2)]
    return lax.ppermute(value, GRID, pairs)


def swapped(value):
    return lax.ppermute(value, "c", [(0, 1), (1, 0)])


def gathered(found):
    found = found + swapped(found)
    total = found
    for dx, dy in ((1, 0), (0, 1), (1, 1)):
        pairs = [
            (chip(1, xp, 1, yp), chip(1, (xp + dx) % 2, 1, (yp + dy) % 2))
            for xp in range(2)
            for yp in range(2)
        ]
        total = total + lax.ppermute(found, GRID, pairs)
    found = total
    for by in range(1, 4):
        pairs = [
            (4 * chip(1, xp, 1, yp) + z, 4 * chip(1, xp, 1, yp) + (z + by) % 4)
            for xp in range(2)
            for yp in range(2)
            for z in range(4)
        ]
        total = total + lax.ppermute(found, (*GRID, "z"), pairs)
    parts = [total]
    for s, q in ((0, 1), (1, 0), (0, 0)):
        pairs = [
            (chip(1, xp, 1, yp), chip(s, (xp + 1 + s) % 2, q, (yp + 1 + q) % 2))
            for xp in range(2)
            for yp in range(2)
        ]
        parts.append(lax.ppermute(total, GRID, pairs))
    return parts


def body(layout, assign, edge, gate_left, gate_right, phase_angle, close):
    cosine, sine = jnp.cos(phase_angle), jnp.sin(phase_angle)
    cosine = jnp.concatenate([cosine, cosine], -1)
    sine = jnp.concatenate([-sine, sine], -1)
    hbm = pl.BlockSpec(memory_space=pltpu.HBM)
    packed = call(
        pack_kernel,
        shape(8, BLOCK, 2 * W),
        [
            pltpu.SMEM((1, 16), jnp.int32),
            pltpu.SMEM((1, 4), jnp.int32),
            pltpu.VMEM((16, W, 2 * W), BF16),
            pltpu.SemaphoreType.DMA((18,)),
        ],
        [
            pltpu.with_memory_space_constraint(x, pltpu.HBM)
            for x in (layout.T, assign.T, gate_left, gate_right)
        ],
        [hbm, hbm, hbm, hbm],
    )
    mine = lax.all_to_all(packed, ("xp", "q", "yp"), 0, 0, tiled=True)
    other = swapped(mine)
    state = pltpu.VMEM((NR, W, 2 * W), F32)
    peaks = pltpu.VMEM((NC, 2 * W), F32)
    gates = (shape(NC, NR, W, 2 * W, dtype=BF16), shape(NC, NR, 2 * W, 2 * W, dtype=BF16))
    lefts, rights, phases = call(
        unpack_kernel, (*gates, shape(2 * NC, 2 * W)), [], (mine, cosine, sine)
    )
    lefts, rights, board, halo = call(
        first_kernel,
        (*gates, shape(BOARD, 2 * W), shape(HALO, 2 * W)),
        [state, peaks],
        (other, lefts, rights, phases, edge),
        aliases={1: 0, 2: 1},
    )
    board, halo = along_columns(board, 0), along_rows(halo, 0)
    board, halo = call(
        second_kernel,
        (shape(BOARD, 2 * W), shape(HALO, 2 * W)),
        [state, peaks],
        (phases, edge, lefts, rights, close, board, halo),
    )
    board, halo = along_columns(board, 1), along_rows(halo, 1)
    found = call(
        third_kernel,
        shape(8, 2 * W),
        [state, peaks, pltpu.VMEM((HALO, 2 * W), F32)],
        (phases, edge, lefts, rights, close, board, halo),
    )
    amps, logs, total_amp, top_log = call(
        finish_kernel,
        (shape(2, 4), shape(1, 4), shape(1, 2), shape(1, 1)),
        [],
        gathered(found),
    )
    return (amps.T, logs.reshape(4), total_amp.reshape(2), top_log.reshape(()))


def solution(mesh):
    split = Mesh(mesh.devices.reshape(2, 2, 2, 2, 4, 2), AXES)
    placed = (
        P(None, GRID),
        P(("z", "c"), GRID),
        P(),
        P(GRID, None, None, None),
        P(GRID, None, None, None),
        P(),
        P(),
    )
    return jax.shard_map(
        body,
        mesh=split,
        in_specs=placed,
        out_specs=(P(("z", "c"), None), P(("z", "c")), P(), P()),
        check_vma=False,
    )
```

```python
import math

import jax
import jax.numpy as jnp
from jax import lax
from jax.experimental import pallas as pl
from jax.experimental.pallas import tpu as pltpu
from jax.sharding import Mesh
from jax.sharding import PartitionSpec as P

AXES = ("s", "xp", "q", "yp", "z", "c")
GRID = ("s", "xp", "q", "yp")
NC = 8
NR = 8
W = 64
BLOCK = 4 * 2 * W + 8
BOARD = NR * W + 8
HALO = NC * W + 16
F32 = jnp.float32
BF16 = jnp.bfloat16


def vmem():
    return pl.BlockSpec(memory_space=pltpu.VMEM)


def sign_row():
    lane = lax.broadcasted_iota(jnp.int32, (1, 2 * W), 1)
    return jnp.where(lane < W, -1.0, 1.0).astype(F32)


def times_i(x, sign):
    return pltpu.roll(x, W, 1) * sign


def pack_kernel(layout_hbm, assign_hbm, left, right, out, layout, assign, raw, sems):
    core = lax.axis_index("c")
    small = [
        pltpu.make_async_copy(layout_hbm, layout, sems.at[16]),
        pltpu.make_async_copy(assign_hbm, assign, sems.at[17]),
    ]
    for copy in small:
        copy.start()
    for copy in small:
        copy.wait()
    copies = []
    for half in range(2):
        for k in range(4):
            kind = layout[0, (1 - half) * NR + 4 * core + k]
            for side, table in ((0, left), (1, right)):
                n = 8 * half + 2 * k + side
                copies.append(pltpu.make_async_copy(table.at[0, kind], raw.at[n], sems.at[n]))
                copies[-1].start()
    for t in range(4):
        row = jnp.full((1, 2 * W), assign[0, t].astype(F32), F32)
        for dest in range(8):
            out[dest, pl.ds(8 * W + t, 1), :] = row
    for dest in range(8):
        out[dest, pl.ds(8 * W + 4, 4), :] = jnp.zeros((4, 2 * W), F32)
    for n in range(16):
        copies[n].wait()
        x = raw[n].astype(F32)
        half, row = n // 8, n % 8
        for xp in range(2):
            for yp in range(2):
                out[4 * xp + 2 * half + yp, pl.ds(W * row, W), :] = x


def unpack(source, part, lefts, rights, sign):
    def place(j, unused):
        for k in range(4):
            row = 4 * part + k
            lefts[j, row] = source[j, pl.ds(2 * W * k, W), :].astype(BF16)
            r = source[j, pl.ds(2 * W * k + W, W), :]
            rights[j, row, pl.ds(0, W), :] = r.astype(BF16)
            rights[j, row, pl.ds(W, W), :] = times_i(r, sign).astype(BF16)
        return unused

    lax.fori_loop(0, NC, place, 0)


def unpack_kernel(mine, cosine, sine, lefts, rights, phases):
    s, q, own, base = places()
    unpack(mine, lax.axis_index("c"), lefts, rights, sign_row())
    for j in range(NC):
        value = mine[j, pl.ds(8 * W + own, 1), :]
        for n, table in ((0, cosine), (NC, sine)):
            row = jnp.zeros((1, 2 * W), F32)
            for v in range(4):
                row = jnp.where(value == float(v), table[pl.ds(v, 1), :], row)
            phases[pl.ds(n + j, 1), :] = row


def halves(x):
    high = x.astype(BF16)
    return high, (x - high.astype(F32)).astype(BF16)


def sweep(state, lefts, rights, phases, halo_in, halo_out, peaks, start, sign):
    def column(j, carry):
        p, rho_mix, rho = carry
        scale = 1.0 / p
        cos_row = phases[pl.ds(j, 1), :] * scale
        sin_row = phases[pl.ds(NC + j, 1), :] * scale
        boards = [state[k] for k in range(NR)]
        halo_out[pl.ds(j * W, W), :] = boards[0]
        if halo_in is None:
            below = None
        else:
            below = halo_in[pl.ds(j * W, W), :] * rho_mix
        top = jnp.zeros((8, 2 * W), F32)
        for k in range(NR):
            after = boards[k + 1] if k + 1 < NR else below
            mixed = boards[k] if after is None else boards[k] + 0.5 * after
            turn = times_i(mixed, sign)
            mh, ml = halves(mixed)
            th, tl = halves(turn)
            both = jnp.dot(
                lefts[j, k],
                jnp.concatenate([jnp.concatenate([mh, th], 0), jnp.concatenate([ml, tl], 0)], 1),
                preferred_element_type=F32,
            )
            middle = both[:, : 2 * W] + both[:, 2 * W :]
            dh, dl = halves(middle)
            two = jnp.dot(
                jnp.concatenate([dh, dl], 0), rights[j, k], preferred_element_type=F32
            )
            out = two[:W] + two[W:]
            out = out * cos_row + pltpu.roll(out, W, 1) * sin_row
            state[k] = out
            for g in range(8):
                top = jnp.maximum(top, jnp.abs(out[8 * g : 8 * g + 8]))
        own_top = jnp.broadcast_to(jnp.max(top, keepdims=True), (1, 2 * W))
        halo_out[pl.ds(NC * W + j, 1), :] = own_top
        if halo_in is None:
            other_top = jnp.zeros((1, 2 * W), F32)
        else:
            other_top = halo_in[pl.ds(NC * W + j, 1), :]
        p_new = jnp.maximum(jnp.maximum(own_top, other_top * rho), 1.0)
        peaks[pl.ds(j, 1), :] = p_new
        return (p_new, rho, rho * jnp.maximum(other_top, 1.0) / p_new)

    carry = start
    for j in range(NC):
        carry = column(j, carry)
    return carry


def close_sums(state, close, base, sign):
    real = jnp.zeros((8, 2 * W), F32)
    imag = jnp.zeros((8, 2 * W), F32)
    for k in range(NR):
        c = close[base + k]
        b = state[k]
        d = pltpu.roll(c, W, 1)
        for g in range(8):
            part = slice(8 * g, 8 * g + 8)
            real = real - b[part] * c[part] * sign
            imag = imag + b[part] * d[part]
    return jnp.sum(real, keepdims=True), jnp.sum(imag, keepdims=True)


def write_messages(state, board_out, halo_out, peaks, ell, end, sums):
    p, rho_mix, rho = end
    for k in range(NR):
        board_out[pl.ds(k * W, W), :] = state[k]
    board_out[pl.ds(NR * W, 1), :] = p
    board_out[pl.ds(NR * W + 1, 1), :] = rho_mix
    board_out[pl.ds(NR * W + 2, 1), :] = rho
    board_out[pl.ds(NR * W + 3, 1), :] = ell + jnp.sum(jnp.log(peaks[...]), axis=0, keepdims=True)
    board_out[pl.ds(NR * W + 4, 4), :] = jnp.zeros((4, 2 * W), F32)
    halo_out[pl.ds(NC * W + 8, 8), :] = jnp.zeros((8, 2 * W), F32)
    if sums is not None:
        halo_out[pl.ds(NC * W + 8, 1), :] = jnp.broadcast_to(sums[0], (1, 2 * W))
        halo_out[pl.ds(NC * W + 9, 1), :] = jnp.broadcast_to(sums[1], (1, 2 * W))


def places():
    s, q = lax.axis_index("s"), lax.axis_index("q")
    i = jnp.where(s == 0, lax.axis_index("xp"), 1 - lax.axis_index("xp"))
    j = jnp.where(q == 0, lax.axis_index("yp"), 1 - lax.axis_index("yp"))
    return s, q, 2 * i + j, (1 - q) * NR


def first_kernel(other, lefts_in, rights_in, phases, edge, lefts, rights, board_out, halo_out, state, peaks):
    s, q, own, base = places()
    sign = sign_row()
    one = jnp.ones((1, 2 * W), F32)
    unpack(other, 1 - lax.axis_index("c"), lefts, rights, sign)
    for k in range(NR):
        state[k] = edge[base + k].astype(F32)
    end = sweep(state, lefts, rights, phases, None, halo_out, peaks, (one, one, one), sign)
    write_messages(state, board_out, halo_out, peaks, 0.0 * one, end, None)


def load_state(state, edge, board_in, base, s):
    one = jnp.ones((1, 2 * W), F32)
    first = s == 0
    for k in range(NR):
        state[k] = jnp.where(first, edge[base + k].astype(F32), board_in[pl.ds(k * W, W), :])
    row = lambda n: board_in[pl.ds(NR * W + n, 1), :]
    p = jnp.maximum(jnp.where(first, one, row(0)), 1.0)
    rho_mix = jnp.where(first, one, row(1))
    rho = jnp.where(first, one, row(2))
    ell = jnp.where(first, 0.0 * one, row(3))
    return (p, rho_mix, rho), ell


def second_kernel(phases, edge, lefts, rights, close, board_in, halo_in, board_out, halo_out, state, peaks):
    s, q, own, base = places()
    sign = sign_row()
    start, ell = load_state(state, edge, board_in, base, s)
    end = sweep(state, lefts, rights, phases, halo_in, halo_out, peaks, start, sign)
    write_messages(
        state, board_out, halo_out, peaks, ell, end, close_sums(state, close, base, sign)
    )


def third_kernel(phases, edge, lefts, rights, close, board_in, halo_in, out, state, peaks, halo_out):
    s, q, own, base = places()
    sign = sign_row()
    start, ell = load_state(state, edge, board_in, base, s)
    p, rho_mix, rho = sweep(state, lefts, rights, phases, halo_in, halo_out, peaks, start, sign)
    ell = ell + jnp.sum(jnp.log(peaks[...]), axis=0, keepdims=True)
    real, imag = close_sums(state, close, base, sign)
    factor = 1.0 / math.sqrt(2 * NR * W * W)
    real = (real + rho_mix * halo_in[pl.ds(NC * W + 8, 1), :]) / p * factor
    imag = (imag + rho_mix * halo_in[pl.ds(NC * W + 9, 1), :]) / p * factor
    index = 4 * (2 * lax.axis_index("z") + lax.axis_index("c")) + own
    lane = lax.broadcasted_iota(jnp.int32, (1, 2 * W), 1)
    index = jnp.where(jnp.logical_and(s == 1, q == 1), index, -1)
    hit = lane == index
    zero = jnp.zeros((1, 2 * W), F32)
    out[pl.ds(0, 1), :] = jnp.where(hit, real, zero)
    out[pl.ds(1, 1), :] = jnp.where(hit, imag, zero)
    out[pl.ds(2, 1), :] = jnp.where(hit, ell, zero)
    out[pl.ds(3, 5), :] = jnp.zeros((5, 2 * W), F32)


def finish_kernel(blocks, amps, logs, total, top):
    found = jnp.sum(blocks[...], axis=0)
    ell = found[2:3]
    high = jnp.max(ell, axis=1, keepdims=True)
    weighted = found[0:2] * jnp.exp(ell - high)
    top[...] = high
    sums = jnp.sum(weighted, axis=1, keepdims=True)
    total[...] = jnp.concatenate([sums[0:1], sums[1:2]], 1)
    at = 4 * (2 * lax.axis_index("z") + lax.axis_index("c"))
    here = pltpu.roll(found, jnp.where(at == 0, 0, 2 * W - at), 1)
    amps[...] = here[0:2, 0:4]
    logs[...] = here[2:3, 0:4]


def call(kernel, outs, scratch, args, specs=None, aliases=None):
    return pl.pallas_call(
        kernel,
        out_shape=outs,
        in_specs=specs or [vmem()] * len(args),
        out_specs=jax.tree.map(lambda _: vmem(), outs),
        scratch_shapes=scratch,
        input_output_aliases=aliases or {},
        compiler_params=pltpu.CompilerParams(vmem_limit_bytes=20 * 2**20),
    )(*args)


def shape(*dims, dtype=F32):
    return jax.ShapeDtypeStruct(dims, dtype)


def chip(s, xp, q, yp):
    return 8 * s + 4 * xp + 2 * q + yp


def along_columns(value, q):
    pairs = [(chip(0, xp, q, yp), chip(1, 1 - xp, q, yp)) for xp in range(2) for yp in range(2)]
    return lax.ppermute(value, GRID, pairs)


def along_rows(value, s):
    pairs = [(chip(s, xp, 0, yp), chip(s, xp, 1, 1 - yp)) for xp in range(2) for yp in range(2)]
    return lax.ppermute(value, GRID, pairs)


def swapped(value):
    return lax.ppermute(value, "c", [(0, 1), (1, 0)])


def gathered(found):
    found = found + swapped(found)
    chips = (*GRID, "z")
    count = lax.axis_size(chips)
    spread = jnp.broadcast_to(found[None], (count, *found.shape))
    return lax.all_to_all(spread, chips, 0, 0, tiled=True)


def body(layout, assign, edge, gate_left, gate_right, phase_angle, close):
    cosine, sine = jnp.cos(phase_angle), jnp.sin(phase_angle)
    cosine = jnp.concatenate([cosine, cosine], -1)
    sine = jnp.concatenate([-sine, sine], -1)
    hbm = pl.BlockSpec(memory_space=pltpu.HBM)
    packed = call(
        pack_kernel,
        shape(8, BLOCK, 2 * W),
        [
            pltpu.SMEM((1, 16), jnp.int32),
            pltpu.SMEM((1, 4), jnp.int32),
            pltpu.VMEM((16, W, 2 * W), BF16),
            pltpu.SemaphoreType.DMA((18,)),
        ],
        [
            pltpu.with_memory_space_constraint(x, pltpu.HBM)
            for x in (layout.T, assign.T, gate_left, gate_right)
        ],
        [hbm, hbm, hbm, hbm],
    )
    mine = lax.all_to_all(packed, ("xp", "q", "yp"), 0, 0, tiled=True)
    other = swapped(mine)
    state = pltpu.VMEM((NR, W, 2 * W), F32)
    peaks = pltpu.VMEM((NC, 2 * W), F32)
    gates = (shape(NC, NR, W, 2 * W, dtype=BF16), shape(NC, NR, 2 * W, 2 * W, dtype=BF16))
    lefts, rights, phases = call(
        unpack_kernel, (*gates, shape(2 * NC, 2 * W)), [], (mine, cosine, sine)
    )
    lefts, rights, board, halo = call(
        first_kernel,
        (*gates, shape(BOARD, 2 * W), shape(HALO, 2 * W)),
        [state, peaks],
        (other, lefts, rights, phases, edge),
        aliases={1: 0, 2: 1},
    )
    board, halo = along_columns(board, 0), along_rows(halo, 0)
    board, halo = call(
        second_kernel,
        (shape(BOARD, 2 * W), shape(HALO, 2 * W)),
        [state, peaks],
        (phases, edge, lefts, rights, close, board, halo),
    )
    board, halo = along_columns(board, 1), along_rows(halo, 1)
    found = call(
        third_kernel,
        shape(8, 2 * W),
        [state, peaks, pltpu.VMEM((HALO, 2 * W), F32)],
        (phases, edge, lefts, rights, close, board, halo),
    )
    amps, logs, total_amp, top_log = call(
        finish_kernel,
        (shape(2, 4), shape(1, 4), shape(1, 2), shape(1, 1)),
        [],
        (gathered(found),),
    )
    return (amps.T, logs.reshape(4), total_amp.reshape(2), top_log.reshape(()))


def solution(mesh):
    split = Mesh(mesh.devices.reshape(2, 2, 2, 2, 4, 2), AXES)
    placed = (
        P(None, GRID),
        P(("z", "c"), GRID),
        P(),
        P(GRID, None, None, None),
        P(GRID, None, None, None),
        P(),
        P(),
    )
    return jax.shard_map(
        body,
        mesh=split,
        in_specs=placed,
        out_specs=(P(("z", "c"), None), P(("z", "c")), P(), P()),
        check_vma=False,
    )
```

```python
import math

import jax
import jax.numpy as jnp
from jax import lax
from jax.experimental import pallas as pl
from jax.experimental.pallas import tpu as pltpu
from jax.sharding import Mesh
from jax.sharding import PartitionSpec as P

AXES = ("s", "xp", "yh", "q", "z", "c")
GRID = ("s", "xp", "yh", "q")
NC = 8
NR = 8
W = 64
BLOCK = 4 * 2 * W + 8
BOARD = NR * W + 8
HALO = NC * W + 16
F32 = jnp.float32
BF16 = jnp.bfloat16


def vmem():
    return pl.BlockSpec(memory_space=pltpu.VMEM)


def sign_row():
    lane = lax.broadcasted_iota(jnp.int32, (1, 2 * W), 1)
    return jnp.where(lane < W, -1.0, 1.0).astype(F32)


def times_i(x, sign):
    return pltpu.roll(x, W, 1) * sign


def pack_kernel(layout_hbm, assign_hbm, left, right, out, layout, assign, raw, sems):
    core = lax.axis_index("c")
    small = [
        pltpu.make_async_copy(layout_hbm, layout, sems.at[16]),
        pltpu.make_async_copy(assign_hbm, assign, sems.at[17]),
    ]
    for copy in small:
        copy.start()
    for copy in small:
        copy.wait()
    copies = []
    for half in range(2):
        for k in range(4):
            kind = layout[0, (1 - half) * NR + 4 * core + k]
            for side, table in ((0, left), (1, right)):
                n = 8 * half + 2 * k + side
                copies.append(pltpu.make_async_copy(table.at[0, kind], raw.at[n], sems.at[n]))
                copies[-1].start()
    for t in range(4):
        row = jnp.full((1, 2 * W), assign[0, t].astype(F32), F32)
        for dest in range(8):
            out[dest, pl.ds(8 * W + t, 1), :] = row
    for dest in range(8):
        out[dest, pl.ds(8 * W + 4, 4), :] = jnp.zeros((4, 2 * W), F32)
    for n in range(16):
        copies[n].wait()
        x = raw[n].astype(F32)
        half, row = n // 8, n % 8
        for dest in range(half, 8, 2):
            out[dest, pl.ds(W * row, W), :] = x


def unpack(source, part, lefts, rights, sign):
    def place(j, unused):
        for k in range(4):
            row = 4 * part + k
            lefts[j, row] = source[j, pl.ds(2 * W * k, W), :].astype(BF16)
            r = source[j, pl.ds(2 * W * k + W, W), :]
            rights[j, row, pl.ds(0, W), :] = r.astype(BF16)
            rights[j, row, pl.ds(W, W), :] = times_i(r, sign).astype(BF16)
        return unused

    lax.fori_loop(0, NC, place, 0)


def unpack_kernel(mine, cosine, sine, lefts, rights, phases):
    s, q, own, base = places()
    unpack(mine, lax.axis_index("c"), lefts, rights, sign_row())
    for j in range(NC):
        value = mine[j, pl.ds(8 * W + own, 1), :]
        for n, table in ((0, cosine), (NC, sine)):
            row = jnp.zeros((1, 2 * W), F32)
            for v in range(4):
                row = jnp.where(value == float(v), table[pl.ds(v, 1), :], row)
            phases[pl.ds(n + j, 1), :] = row


def halves(x):
    high = x.astype(BF16)
    return high, (x - high.astype(F32)).astype(BF16)


def sweep(state, turned, lefts, rights, phases, halo_in, halo_out, peaks, start, sign):
    def column(j, carry):
        p, rho_mix, rho = carry
        scale = 1.0 / p
        cos_row = phases[pl.ds(j, 1), :] * scale
        sin_row = phases[pl.ds(NC + j, 1), :] * scale
        cos_turn = cos_row * sign
        sin_turn = sin_row * sign
        boards = [state[k] for k in range(NR)]
        turns = [turned[k] for k in range(NR)]
        halo_out[pl.ds(j * W, W), :] = boards[0]
        if halo_in is None:
            below = below_turn = None
        else:
            below = halo_in[pl.ds(j * W, W), :] * rho_mix
            below_turn = times_i(below, sign)
        top = jnp.zeros((8, 2 * W), F32)
        for k in range(NR):
            after = boards[k + 1] if k + 1 < NR else below
            mixed = boards[k] if after is None else boards[k] + 0.5 * after
            after = turns[k + 1] if k + 1 < NR else below_turn
            turn = turns[k] if after is None else turns[k] + 0.5 * after
            mh, ml = halves(mixed)
            th, tl = halves(turn)
            both = jnp.dot(
                lefts[j, k],
                jnp.concatenate([jnp.concatenate([mh, th], 0), jnp.concatenate([ml, tl], 0)], 1),
                preferred_element_type=F32,
            )
            middle = both[:, : 2 * W] + both[:, 2 * W :]
            dh, dl = halves(middle)
            two = jnp.dot(
                jnp.concatenate([dh, dl], 0), rights[j, k], preferred_element_type=F32
            )
            plain = two[:W] + two[W:]
            flip = pltpu.roll(plain, W, 1)
            out = plain * cos_row + flip * sin_row
            state[k] = out
            turned[k] = flip * cos_turn - plain * sin_turn
            for g in range(8):
                top = jnp.maximum(top, jnp.abs(out[8 * g : 8 * g + 8]))
        own_top = jnp.broadcast_to(jnp.max(top, keepdims=True), (1, 2 * W))
        halo_out[pl.ds(NC * W + j, 1), :] = own_top
        if halo_in is None:
            other_top = jnp.zeros((1, 2 * W), F32)
        else:
            other_top = halo_in[pl.ds(NC * W + j, 1), :]
        p_new = jnp.maximum(jnp.maximum(own_top, other_top * rho), 1.0)
        peaks[pl.ds(j, 1), :] = p_new
        return (p_new, rho, rho * jnp.maximum(other_top, 1.0) / p_new)

    carry = start
    for j in range(NC):
        carry = column(j, carry)
    return carry


def close_sums(state, close, base, sign):
    real = jnp.zeros((8, 2 * W), F32)
    imag = jnp.zeros((8, 2 * W), F32)
    for k in range(NR):
        c = close[base + k]
        b = state[k]
        d = pltpu.roll(c, W, 1)
        for g in range(8):
            part = slice(8 * g, 8 * g + 8)
            real = real - b[part] * c[part] * sign
            imag = imag + b[part] * d[part]
    return jnp.sum(real, keepdims=True), jnp.sum(imag, keepdims=True)


def write_messages(state, board_out, halo_out, peaks, ell, end, sums):
    p, rho_mix, rho = end
    for k in range(NR):
        board_out[pl.ds(k * W, W), :] = state[k]
    board_out[pl.ds(NR * W, 1), :] = p
    board_out[pl.ds(NR * W + 1, 1), :] = rho_mix
    board_out[pl.ds(NR * W + 2, 1), :] = rho
    board_out[pl.ds(NR * W + 3, 1), :] = ell + jnp.sum(jnp.log(peaks[...]), axis=0, keepdims=True)
    board_out[pl.ds(NR * W + 4, 4), :] = jnp.zeros((4, 2 * W), F32)
    halo_out[pl.ds(NC * W + 8, 8), :] = jnp.zeros((8, 2 * W), F32)
    if sums is not None:
        halo_out[pl.ds(NC * W + 8, 1), :] = jnp.broadcast_to(sums[0], (1, 2 * W))
        halo_out[pl.ds(NC * W + 9, 1), :] = jnp.broadcast_to(sums[1], (1, 2 * W))


def places():
    s, q = lax.axis_index("s"), lax.axis_index("q")
    i = jnp.where(s == 0, lax.axis_index("xp"), 1 - lax.axis_index("xp"))
    stays = jnp.logical_or(q == 0, lax.axis_index("c") == 1)
    j = jnp.where(stays, lax.axis_index("yh"), 1 - lax.axis_index("yh"))
    return s, q, 2 * i + j, (1 - q) * NR


def first_kernel(other, lefts_in, rights_in, phases, edge, lefts, rights, board_out, halo_out, state, turned, peaks):
    s, q, own, base = places()
    sign = sign_row()
    one = jnp.ones((1, 2 * W), F32)
    unpack(other, 1 - lax.axis_index("c"), lefts, rights, sign)
    for k in range(NR):
        state[k] = edge[base + k].astype(F32)
        turned[k] = times_i(state[k], sign)
    end = sweep(state, turned, lefts, rights, phases, None, halo_out, peaks, (one, one, one), sign)
    write_messages(state, board_out, halo_out, peaks, 0.0 * one, end, None)


def load_state(state, turned, edge, board_in, base, s, sign):
    one = jnp.ones((1, 2 * W), F32)
    first = s == 0
    for k in range(NR):
        x = jnp.where(first, edge[base + k].astype(F32), board_in[pl.ds(k * W, W), :])
        state[k] = x
        turned[k] = times_i(x, sign)
    row = lambda n: board_in[pl.ds(NR * W + n, 1), :]
    p = jnp.maximum(jnp.where(first, one, row(0)), 1.0)
    rho_mix = jnp.where(first, one, row(1))
    rho = jnp.where(first, one, row(2))
    ell = jnp.where(first, 0.0 * one, row(3))
    return (p, rho_mix, rho), ell


def second_kernel(phases, edge, lefts, rights, close, board_in, halo_in, board_out, halo_out, state, turned, peaks):
    s, q, own, base = places()
    sign = sign_row()
    start, ell = load_state(state, turned, edge, board_in, base, s, sign)
    end = sweep(state, turned, lefts, rights, phases, halo_in, halo_out, peaks, start, sign)
    write_messages(
        state, board_out, halo_out, peaks, ell, end, close_sums(state, close, base, sign)
    )


def third_kernel(phases, edge, lefts, rights, close, board_in, halo_in, out, state, turned, peaks, halo_out):
    s, q, own, base = places()
    sign = sign_row()
    start, ell = load_state(state, turned, edge, board_in, base, s, sign)
    p, rho_mix, rho = sweep(state, turned, lefts, rights, phases, halo_in, halo_out, peaks, start, sign)
    ell = ell + jnp.sum(jnp.log(peaks[...]), axis=0, keepdims=True)
    real, imag = close_sums(state, close, base, sign)
    factor = 1.0 / math.sqrt(2 * NR * W * W)
    real = (real + rho_mix * halo_in[pl.ds(NC * W + 8, 1), :]) / p * factor
    imag = (imag + rho_mix * halo_in[pl.ds(NC * W + 9, 1), :]) / p * factor
    index = 4 * (2 * lax.axis_index("z") + lax.axis_index("c")) + own
    lane = lax.broadcasted_iota(jnp.int32, (1, 2 * W), 1)
    index = jnp.where(jnp.logical_and(s == 1, q == 1), index, -128)
    row = jnp.where(lane == index, real, 0.0)
    row = row + jnp.where(lane == index + 32, imag, 0.0)
    row = row + jnp.where(lane == index + 64, ell, 0.0)
    out[...] = row


def finish_kernel(blocks, amps, logs, total, top):
    found = jnp.sum(blocks[...], axis=0, keepdims=True)
    real, imag, ell = found, pltpu.roll(found, 96, 1), pltpu.roll(found, 64, 1)
    used = lax.broadcasted_iota(jnp.int32, (1, 2 * W), 1) < 32
    high = jnp.max(jnp.where(used, ell, 0.0), axis=1, keepdims=True)
    weight = jnp.where(used, jnp.exp(jnp.where(used, ell - high, 0.0)), 0.0)
    top[...] = high
    sums = [jnp.sum(x * weight, axis=1, keepdims=True) for x in (real, imag)]
    total[...] = jnp.concatenate(sums, 1)
    at = 4 * (2 * lax.axis_index("z") + lax.axis_index("c"))
    shift = jnp.where(at == 0, 0, 2 * W - at)
    amps[0:1, :] = pltpu.roll(real, shift, 1)[:, 0:4]
    amps[1:2, :] = pltpu.roll(imag, shift, 1)[:, 0:4]
    logs[...] = pltpu.roll(ell, shift, 1)[:, 0:4]


def call(kernel, outs, scratch, args, specs=None, aliases=None):
    return pl.pallas_call(
        kernel,
        out_shape=outs,
        in_specs=specs or [vmem()] * len(args),
        out_specs=jax.tree.map(lambda _: vmem(), outs),
        scratch_shapes=scratch,
        input_output_aliases=aliases or {},
        compiler_params=pltpu.CompilerParams(vmem_limit_bytes=20 * 2**20),
    )(*args)


def shape(*dims, dtype=F32):
    return jax.ShapeDtypeStruct(dims, dtype)


def chip(s, xp, yh, q):
    return 8 * s + 4 * xp + 2 * yh + q


def along_columns(value, q):
    pairs = [(chip(0, xp, yh, q), chip(1, 1 - xp, yh, q)) for xp in range(2) for yh in range(2)]
    return lax.ppermute(value, GRID, pairs)


def along_rows(value, s):
    pairs = []
    for xp in range(2):
        for yh in range(2):
            source = 2 * chip(s, xp, yh, 0)
            pairs.append((source, 2 * chip(s, xp, 1 - yh, 1)))
            pairs.append((source + 1, 2 * chip(s, xp, yh, 1) + 1))
    return lax.ppermute(value, (*GRID, "c"), pairs)


def swapped(value):
    return lax.ppermute(value, "c", [(0, 1), (1, 0)])


def gathered(found):
    count = lax.axis_size(AXES)
    spread = jnp.broadcast_to(found[None], (count, *found.shape))
    return lax.all_to_all(spread, AXES, 0, 0, tiled=True).reshape(count, found.shape[1])


def body(layout, assign, edge, gate_left, gate_right, phase_angle, close):
    cosine, sine = jnp.cos(phase_angle), jnp.sin(phase_angle)
    cosine = jnp.concatenate([cosine, cosine], -1)
    sine = jnp.concatenate([-sine, sine], -1)
    hbm = pl.BlockSpec(memory_space=pltpu.HBM)
    packed = call(
        pack_kernel,
        shape(8, BLOCK, 2 * W),
        [
            pltpu.SMEM((1, 16), jnp.int32),
            pltpu.SMEM((1, 4), jnp.int32),
            pltpu.VMEM((16, W, 2 * W), BF16),
            pltpu.SemaphoreType.DMA((18,)),
        ],
        [
            pltpu.with_memory_space_constraint(x, pltpu.HBM)
            for x in (layout.T, assign.T, gate_left, gate_right)
        ],
        [hbm, hbm, hbm, hbm],
    )
    mine = lax.all_to_all(packed, ("xp", "yh", "q"), 0, 0, tiled=True)
    other = swapped(mine)
    state = pltpu.VMEM((NR, W, 2 * W), F32)
    peaks = pltpu.VMEM((NC, 2 * W), F32)
    gates = (shape(NC, NR, W, 2 * W, dtype=BF16), shape(NC, NR, 2 * W, 2 * W, dtype=BF16))
    lefts, rights, phases = call(
        unpack_kernel, (*gates, shape(2 * NC, 2 * W)), [], (mine, cosine, sine)
    )
    lefts, rights, board, halo = call(
        first_kernel,
        (*gates, shape(BOARD, 2 * W), shape(HALO, 2 * W)),
        [state, state, peaks],
        (other, lefts, rights, phases, edge),
        aliases={1: 0, 2: 1},
    )
    board, halo = along_columns(board, 0), along_rows(halo, 0)
    board, halo = call(
        second_kernel,
        (shape(BOARD, 2 * W), shape(HALO, 2 * W)),
        [state, state, peaks],
        (phases, edge, lefts, rights, close, board, halo),
    )
    board, halo = along_columns(board, 1), along_rows(halo, 1)
    found = call(
        third_kernel,
        shape(1, 2 * W),
        [state, state, peaks, pltpu.VMEM((HALO, 2 * W), F32)],
        (phases, edge, lefts, rights, close, board, halo),
    )
    amps, logs, total_amp, top_log = call(
        finish_kernel,
        (shape(2, 4), shape(1, 4), shape(1, 2), shape(1, 1)),
        [],
        (gathered(found),),
    )
    return (amps.T, logs.reshape(4), total_amp.reshape(2), top_log.reshape(()))


def solution(mesh):
    split = Mesh(mesh.devices.reshape(2, 2, 2, 2, 4, 2), AXES)
    placed = (
        P(None, GRID),
        P(("z", "c"), GRID),
        P(),
        P(GRID, None, None, None),
        P(GRID, None, None, None),
        P(),
        P(),
    )
    return jax.shard_map(
        body,
        mesh=split,
        in_specs=placed,
        out_specs=(P(("z", "c"), None), P(("z", "c")), P(), P()),
        check_vma=False,
    )
```

```python
import math

import jax
import jax.numpy as jnp
from jax import lax
from jax.experimental import pallas as pl
from jax.experimental.pallas import tpu as pltpu
from jax.sharding import Mesh
from jax.sharding import PartitionSpec as P

AXES = ("s", "xp", "yh", "q", "z", "c")
GRID = ("s", "xp", "yh", "q")
NC = 8
NR = 8
W = 64
BLOCK = 4 * 2 * W + 8
BOARD = NR * W + 8
HALO = NC * W + 16
F32 = jnp.float32
BF16 = jnp.bfloat16


def vmem():
    return pl.BlockSpec(memory_space=pltpu.VMEM)


def sign_row():
    lane = lax.broadcasted_iota(jnp.int32, (1, 2 * W), 1)
    return jnp.where(lane < W, -1.0, 1.0).astype(F32)


def times_i(x, sign):
    return pltpu.roll(x, W, 1) * sign


def pack_kernel(layout_hbm, assign_hbm, left_hbm, right_hbm, out, layout, assign, left, right, sems):
    core = lax.axis_index("c")
    copies = [
        pltpu.make_async_copy(layout_hbm, layout, sems.at[0]),
        pltpu.make_async_copy(assign_hbm, assign, sems.at[1]),
        pltpu.make_async_copy(left_hbm, left, sems.at[2]),
        pltpu.make_async_copy(right_hbm, right, sems.at[3]),
    ]
    for copy in copies:
        copy.start()
    for dest in range(8):
        out[dest, pl.ds(8 * W + 4, 4), :] = jnp.zeros((4, 2 * W), F32)
    for copy in copies:
        copy.wait()
    for t in range(4):
        row = jnp.full((1, 2 * W), assign[0, t].astype(F32), F32)
        for dest in range(8):
            out[dest, pl.ds(8 * W + t, 1), :] = row
    for half in range(2):
        for k in range(4):
            kind = layout[0, (1 - half) * NR + 4 * core + k]
            for n, table in ((2 * k, left), (2 * k + 1, right)):
                x = table[0, kind].astype(F32)
                for dest in range(half, 8, 2):
                    out[dest, pl.ds(W * n, W), :] = x


def unpack_column(source, j, part, lefts, rights, sign):
    for k in range(4):
        row = 4 * part + k
        lefts[j, row] = source[j, pl.ds(2 * W * k, W), :].astype(BF16)
        r = source[j, pl.ds(2 * W * k + W, W), :]
        rights[j, row, pl.ds(0, W), :] = r.astype(BF16)
        rights[j, row, pl.ds(W, W), :] = times_i(r, sign).astype(BF16)


def unpack_kernel(mine, cosine, sine, lefts, rights, phases):
    _, _, own, _ = places()
    part, sign = lax.axis_index("c"), sign_row()

    def place(j, unused):
        unpack_column(mine, j, part, lefts, rights, sign)
        return unused

    lax.fori_loop(0, NC, place, 0)
    for j in range(NC):
        value = mine[j, pl.ds(8 * W + own, 1), :]
        for n, table in ((0, cosine), (NC, sine)):
            row = jnp.zeros((1, 2 * W), F32)
            for v in range(4):
                row = jnp.where(value == float(v), table[pl.ds(v, 1), :], row)
            phases[pl.ds(n + j, 1), :] = row


def halves(x):
    high = x.astype(BF16)
    return high, (x - high.astype(F32)).astype(BF16)


def sweep(state, turned, lefts, rights, phases, halo_in, halo_out, peaks, start, sign, prepare=None):
    def column(j, carry):
        p, rho_mix, rho = carry
        scale = 1.0 / p
        cos_row = phases[pl.ds(j, 1), :] * scale
        sin_row = phases[pl.ds(NC + j, 1), :] * scale
        cos_turn = cos_row * sign
        sin_turn = sin_row * sign
        boards = [state[k] for k in range(NR)]
        turns = [turned[k] for k in range(NR)]
        halo_out[pl.ds(j * W, W), :] = boards[0]
        if halo_in is None:
            below = below_turn = None
        else:
            below = halo_in[pl.ds(j * W, W), :] * rho_mix
            below_turn = times_i(below, sign)
        top = jnp.zeros((8, 2 * W), F32)
        for k in range(NR):
            after = boards[k + 1] if k + 1 < NR else below
            mixed = boards[k] if after is None else boards[k] + 0.5 * after
            after = turns[k + 1] if k + 1 < NR else below_turn
            turn = turns[k] if after is None else turns[k] + 0.5 * after
            mh, ml = halves(mixed)
            th, tl = halves(turn)
            both = jnp.dot(
                lefts[j, k],
                jnp.concatenate([jnp.concatenate([mh, th], 0), jnp.concatenate([ml, tl], 0)], 1),
                preferred_element_type=F32,
            )
            middle = both[:, : 2 * W] + both[:, 2 * W :]
            dh, dl = halves(middle)
            two = jnp.dot(
                jnp.concatenate([dh, dl], 0), rights[j, k], preferred_element_type=F32
            )
            plain = two[:W] + two[W:]
            flip = pltpu.roll(plain, W, 1)
            out = plain * cos_row + flip * sin_row
            state[k] = out
            turned[k] = flip * cos_turn - plain * sin_turn
            for g in range(8):
                top = jnp.maximum(top, jnp.abs(out[8 * g : 8 * g + 8]))
        own_top = jnp.broadcast_to(jnp.max(top, keepdims=True), (1, 2 * W))
        halo_out[pl.ds(NC * W + j, 1), :] = own_top
        if halo_in is None:
            other_top = jnp.zeros((1, 2 * W), F32)
        else:
            other_top = halo_in[pl.ds(NC * W + j, 1), :]
        p_new = jnp.maximum(jnp.maximum(own_top, other_top * rho), 1.0)
        peaks[pl.ds(j, 1), :] = p_new
        return (p_new, rho, rho * jnp.maximum(other_top, 1.0) / p_new)

    carry = start
    if prepare is not None:
        prepare(0)
    for j in range(NC):
        if prepare is not None and j + 1 < NC:
            prepare(j + 1)
        carry = column(j, carry)
    return carry


def close_sums(state, close, base, sign):
    real = jnp.zeros((8, 2 * W), F32)
    imag = jnp.zeros((8, 2 * W), F32)
    for k in range(NR):
        c = close[base + k]
        b = state[k]
        d = pltpu.roll(c, W, 1)
        for g in range(8):
            part = slice(8 * g, 8 * g + 8)
            real = real - b[part] * c[part] * sign
            imag = imag + b[part] * d[part]
    return jnp.sum(real, keepdims=True), jnp.sum(imag, keepdims=True)


def write_messages(state, board_out, halo_out, peaks, ell, end, sums):
    p, rho_mix, rho = end
    for k in range(NR):
        board_out[pl.ds(k * W, W), :] = state[k]
    board_out[pl.ds(NR * W, 1), :] = p
    board_out[pl.ds(NR * W + 1, 1), :] = rho_mix
    board_out[pl.ds(NR * W + 2, 1), :] = rho
    board_out[pl.ds(NR * W + 3, 1), :] = ell + jnp.sum(jnp.log(peaks[...]), axis=0, keepdims=True)
    board_out[pl.ds(NR * W + 4, 4), :] = jnp.zeros((4, 2 * W), F32)
    halo_out[pl.ds(NC * W + 8, 8), :] = jnp.zeros((8, 2 * W), F32)
    if sums is not None:
        halo_out[pl.ds(NC * W + 8, 1), :] = jnp.broadcast_to(sums[0], (1, 2 * W))
        halo_out[pl.ds(NC * W + 9, 1), :] = jnp.broadcast_to(sums[1], (1, 2 * W))


def places():
    s, q = lax.axis_index("s"), lax.axis_index("q")
    i = jnp.where(s == 0, lax.axis_index("xp"), 1 - lax.axis_index("xp"))
    stays = jnp.logical_or(q == 0, lax.axis_index("c") == 1)
    j = jnp.where(stays, lax.axis_index("yh"), 1 - lax.axis_index("yh"))
    return s, q, 2 * i + j, (1 - q) * NR


def first_kernel(other, lefts_in, rights_in, phases, edge, lefts, rights, board_out, halo_out, state, turned, peaks):
    _, _, _, base = places()
    sign = sign_row()
    one = jnp.ones((1, 2 * W), F32)
    part = 1 - lax.axis_index("c")
    for k in range(NR):
        state[k] = edge[base + k].astype(F32)
        turned[k] = times_i(state[k], sign)
    prepare = lambda j: unpack_column(other, j, part, lefts, rights, sign)
    end = sweep(
        state, turned, lefts, rights, phases, None, halo_out, peaks, (one, one, one), sign, prepare
    )
    write_messages(state, board_out, halo_out, peaks, 0.0 * one, end, None)


def load_state(state, turned, edge, board_in, base, s, sign):
    one = jnp.ones((1, 2 * W), F32)
    first = s == 0
    for k in range(NR):
        x = jnp.where(first, edge[base + k].astype(F32), board_in[pl.ds(k * W, W), :])
        state[k] = x
        turned[k] = times_i(x, sign)
    row = lambda n: board_in[pl.ds(NR * W + n, 1), :]
    p = jnp.maximum(jnp.where(first, one, row(0)), 1.0)
    rho_mix = jnp.where(first, one, row(1))
    rho = jnp.where(first, one, row(2))
    ell = jnp.where(first, 0.0 * one, row(3))
    return (p, rho_mix, rho), ell


def second_kernel(phases, edge, lefts, rights, close, board_in, halo_in, board_out, halo_out, state, turned, peaks):
    s, _, _, base = places()
    sign = sign_row()
    start, ell = load_state(state, turned, edge, board_in, base, s, sign)
    end = sweep(state, turned, lefts, rights, phases, halo_in, halo_out, peaks, start, sign)
    write_messages(
        state, board_out, halo_out, peaks, ell, end, close_sums(state, close, base, sign)
    )


def third_kernel(phases, edge, lefts, rights, close, board_in, halo_in, out, state, turned, peaks, halo_out):
    s, q, own, base = places()
    sign = sign_row()
    start, ell = load_state(state, turned, edge, board_in, base, s, sign)
    p, rho_mix, _ = sweep(state, turned, lefts, rights, phases, halo_in, halo_out, peaks, start, sign)
    ell = ell + jnp.sum(jnp.log(peaks[...]), axis=0, keepdims=True)
    real, imag = close_sums(state, close, base, sign)
    factor = 1.0 / math.sqrt(2 * NR * W * W)
    real = (real + rho_mix * halo_in[pl.ds(NC * W + 8, 1), :]) / p * factor
    imag = (imag + rho_mix * halo_in[pl.ds(NC * W + 9, 1), :]) / p * factor
    index = 4 * (2 * lax.axis_index("z") + lax.axis_index("c")) + own
    lane = lax.broadcasted_iota(jnp.int32, (1, 2 * W), 1)
    index = jnp.where(jnp.logical_and(s == 1, q == 1), index, -128)
    row = jnp.where(lane == index, real, 0.0)
    row = row + jnp.where(lane == index + 32, imag, 0.0)
    row = row + jnp.where(lane == index + 64, ell, 0.0)
    out[...] = row


def finish_kernel(blocks, amps, logs, total, top):
    found = jnp.sum(blocks[...], axis=0, keepdims=True)
    real, imag, ell = found, pltpu.roll(found, 96, 1), pltpu.roll(found, 64, 1)
    used = lax.broadcasted_iota(jnp.int32, (1, 2 * W), 1) < 32
    high = jnp.max(jnp.where(used, ell, 0.0), axis=1, keepdims=True)
    weight = jnp.where(used, jnp.exp(jnp.where(used, ell - high, 0.0)), 0.0)
    top[...] = high
    sums = [jnp.sum(x * weight, axis=1, keepdims=True) for x in (real, imag)]
    total[...] = jnp.concatenate(sums, 1)
    at = 4 * (2 * lax.axis_index("z") + lax.axis_index("c"))
    shift = jnp.where(at == 0, 0, 2 * W - at)
    amps[0:1, :] = pltpu.roll(real, shift, 1)[:, 0:4]
    amps[1:2, :] = pltpu.roll(imag, shift, 1)[:, 0:4]
    logs[...] = pltpu.roll(ell, shift, 1)[:, 0:4]


def call(kernel, outs, scratch, args, specs=None, aliases=None):
    return pl.pallas_call(
        kernel,
        out_shape=outs,
        in_specs=specs or [vmem()] * len(args),
        out_specs=jax.tree.map(lambda _: vmem(), outs),
        scratch_shapes=scratch,
        input_output_aliases=aliases or {},
        compiler_params=pltpu.CompilerParams(vmem_limit_bytes=20 * 2**20),
    )(*args)


def shape(*dims, dtype=F32):
    return jax.ShapeDtypeStruct(dims, dtype)


def chip(s, xp, yh, q):
    return 8 * s + 4 * xp + 2 * yh + q


def along_columns(value, q):
    pairs = [(chip(0, xp, yh, q), chip(1, 1 - xp, yh, q)) for xp in range(2) for yh in range(2)]
    return lax.ppermute(value, GRID, pairs)


def along_rows(value, s):
    pairs = []
    for xp in range(2):
        for yh in range(2):
            source = 2 * chip(s, xp, yh, 0)
            pairs.append((source, 2 * chip(s, xp, 1 - yh, 1)))
            pairs.append((source + 1, 2 * chip(s, xp, yh, 1) + 1))
    return lax.ppermute(value, (*GRID, "c"), pairs)


def swapped(value):
    return lax.ppermute(value, "c", [(0, 1), (1, 0)])


def gathered(found):
    count = lax.axis_size(AXES)
    spread = jnp.broadcast_to(found[None], (count, *found.shape))
    return lax.all_to_all(spread, AXES, 0, 0, tiled=True).reshape(count, found.shape[1])


def body(layout, assign, edge, gate_left, gate_right, phase_angle, close):
    cosine, sine = jnp.cos(phase_angle), jnp.sin(phase_angle)
    cosine = jnp.concatenate([cosine, cosine], -1)
    sine = jnp.concatenate([-sine, sine], -1)
    hbm = pl.BlockSpec(memory_space=pltpu.HBM)
    packed = call(
        pack_kernel,
        shape(8, BLOCK, 2 * W),
        [
            pltpu.SMEM((1, 16), jnp.int32),
            pltpu.SMEM((1, 4), jnp.int32),
            pltpu.VMEM(gate_left.shape, BF16),
            pltpu.VMEM(gate_right.shape, BF16),
            pltpu.SemaphoreType.DMA((4,)),
        ],
        [
            pltpu.with_memory_space_constraint(x, pltpu.HBM)
            for x in (layout.T, assign.T, gate_left, gate_right)
        ],
        [hbm, hbm, hbm, hbm],
    )
    mine = lax.all_to_all(packed, ("xp", "yh", "q"), 0, 0, tiled=True)
    other = swapped(mine)
    state = pltpu.VMEM((NR, W, 2 * W), F32)
    peaks = pltpu.VMEM((NC, 2 * W), F32)
    gates = (shape(NC, NR, W, 2 * W, dtype=BF16), shape(NC, NR, 2 * W, 2 * W, dtype=BF16))
    lefts, rights, phases = call(
        unpack_kernel, (*gates, shape(2 * NC, 2 * W)), [], (mine, cosine, sine)
    )
    lefts, rights, board, halo = call(
        first_kernel,
        (*gates, shape(BOARD, 2 * W), shape(HALO, 2 * W)),
        [state, state, peaks],
        (other, lefts, rights, phases, edge),
        aliases={1: 0, 2: 1},
    )
    board = along_columns(board, 0)
    halo = along_rows(halo, 0)
    board, halo = call(
        second_kernel,
        (shape(BOARD, 2 * W), shape(HALO, 2 * W)),
        [state, state, peaks],
        (phases, edge, lefts, rights, close, board, halo),
    )
    board, halo = along_columns(board, 1), along_rows(halo, 1)
    found = call(
        third_kernel,
        shape(1, 2 * W),
        [state, state, peaks, pltpu.VMEM((HALO, 2 * W), F32)],
        (phases, edge, lefts, rights, close, board, halo),
    )
    amps, logs, total_amp, top_log = call(
        finish_kernel,
        (shape(2, 4), shape(1, 4), shape(1, 2), shape(1, 1)),
        [],
        (gathered(found),),
    )
    return (amps.T, logs.reshape(4), total_amp.reshape(2), top_log.reshape(()))


def solution(mesh):
    split = Mesh(mesh.devices.reshape(2, 2, 2, 2, 4, 2), AXES)
    placed = (
        P(None, GRID),
        P(("z", "c"), GRID),
        P(),
        P(GRID, None, None, None),
        P(GRID, None, None, None),
        P(),
        P(),
    )
    return jax.shard_map(
        body,
        mesh=split,
        in_specs=placed,
        out_specs=(P(("z", "c"), None), P(("z", "c")), P(), P()),
        check_vma=False,
    )
```

```python
import math

import jax
import jax.numpy as jnp
from jax import lax
from jax.experimental import pallas as pl
from jax.experimental.pallas import tpu as pltpu
from jax.sharding import Mesh
from jax.sharding import PartitionSpec as P

AXES = ("s", "xp", "yh", "q", "z", "c")
GRID = ("s", "xp", "yh", "q")
NC = 8
NR = 8
W = 64
BLOCK = 4 * 2 * W + 8
BOARD = NR * W + 8
HALO = NC * W + 16
F32 = jnp.float32
BF16 = jnp.bfloat16


def vmem():
    return pl.BlockSpec(memory_space=pltpu.VMEM)


def sign_row():
    lane = lax.broadcasted_iota(jnp.int32, (1, 2 * W), 1)
    return jnp.where(lane < W, -1.0, 1.0).astype(F32)


def times_i(x, sign):
    return pltpu.roll(x, W, 1) * sign


def pack_kernel(layout_hbm, assign_hbm, left_hbm, right_hbm, out, layout, assign, left, right, sems):
    core = lax.axis_index("c")
    copies = [
        pltpu.make_async_copy(layout_hbm, layout, sems.at[0]),
        pltpu.make_async_copy(assign_hbm, assign, sems.at[1]),
        pltpu.make_async_copy(left_hbm, left, sems.at[2]),
        pltpu.make_async_copy(right_hbm, right, sems.at[3]),
    ]
    for copy in copies:
        copy.start()
    for dest in range(8):
        out[dest, pl.ds(8 * W + 4, 4), :] = jnp.zeros((4, 2 * W), F32)
    for copy in copies:
        copy.wait()
    for t in range(4):
        row = jnp.full((1, 2 * W), assign[0, t].astype(F32), F32)
        for dest in range(8):
            out[dest, pl.ds(8 * W + t, 1), :] = row
    for half in range(2):
        for k in range(4):
            kind = layout[0, (1 - half) * NR + 4 * core + k]
            for n, table in ((2 * k, left), (2 * k + 1, right)):
                x = table[0, kind].astype(F32)
                for dest in range(half, 8, 2):
                    out[dest, pl.ds(W * n, W), :] = x


def unpack_column(source, j, part, lefts, rights, sign):
    for k in range(4):
        row = 4 * part + k
        lefts[j, row] = source[j, pl.ds(2 * W * k, W), :].astype(BF16)
        r = source[j, pl.ds(2 * W * k + W, W), :]
        rights[j, row, pl.ds(0, W), :] = r.astype(BF16)
        rights[j, row, pl.ds(W, W), :] = times_i(r, sign).astype(BF16)


def unpack_kernel(mine, cosine, sine, lefts, rights, phases):
    _, _, own, _ = places()
    part, sign = lax.axis_index("c"), sign_row()

    def place(j, unused):
        unpack_column(mine, j, part, lefts, rights, sign)
        return unused

    lax.fori_loop(0, NC, place, 0)
    for j in range(NC):
        value = mine[j, pl.ds(8 * W + own, 1), :]
        for n, table in ((0, cosine), (NC, sine)):
            row = jnp.zeros((1, 2 * W), F32)
            for v in range(4):
                row = jnp.where(value == float(v), table[pl.ds(v, 1), :], row)
            phases[pl.ds(n + j, 1), :] = row


def halves(x):
    high = x.astype(BF16)
    return high, (x - high.astype(F32)).astype(BF16)


def sweep(state, turned, lefts, rights, phases, halo_in, halo_out, peaks, start, sign, prepare=None):
    def column(j, carry):
        p, rho_mix, rho = carry
        scale = 1.0 / p
        cos_row = phases[pl.ds(j, 1), :] * scale
        sin_row = phases[pl.ds(NC + j, 1), :] * scale
        cos_turn = cos_row * sign
        sin_turn = sin_row * sign
        boards = [state[k] for k in range(NR)]
        turns = [turned[k] for k in range(NR)]
        halo_out[pl.ds(j * W, W), :] = boards[0]
        if halo_in is None:
            below = below_turn = None
        else:
            below = halo_in[pl.ds(j * W, W), :] * rho_mix
            below_turn = times_i(below, sign)
        top = jnp.zeros((8, 2 * W), F32)
        for k in range(NR):
            after = boards[k + 1] if k + 1 < NR else below
            mixed = boards[k] if after is None else boards[k] + 0.5 * after
            after = turns[k + 1] if k + 1 < NR else below_turn
            turn = turns[k] if after is None else turns[k] + 0.5 * after
            mh, ml = halves(mixed)
            th, tl = halves(turn)
            both = jnp.dot(
                lefts[j, k],
                jnp.concatenate([jnp.concatenate([mh, th], 0), jnp.concatenate([ml, tl], 0)], 1),
                preferred_element_type=F32,
            )
            middle = both[:, : 2 * W] + both[:, 2 * W :]
            dh, dl = halves(middle)
            two = jnp.dot(
                jnp.concatenate([dh, dl], 0), rights[j, k], preferred_element_type=F32
            )
            plain = two[:W] + two[W:]
            flip = pltpu.roll(plain, W, 1)
            out = plain * cos_row + flip * sin_row
            state[k] = out
            turned[k] = flip * cos_turn - plain * sin_turn
            for g in range(8):
                top = jnp.maximum(top, jnp.abs(out[8 * g : 8 * g + 8]))
        own_top = jnp.broadcast_to(jnp.max(top, keepdims=True), (1, 2 * W))
        halo_out[pl.ds(NC * W + j, 1), :] = own_top
        if halo_in is None:
            other_top = jnp.zeros((1, 2 * W), F32)
        else:
            other_top = halo_in[pl.ds(NC * W + j, 1), :]
        p_new = jnp.maximum(jnp.maximum(own_top, other_top * rho), 1.0)
        peaks[pl.ds(j, 1), :] = p_new
        return (p_new, rho, rho * jnp.maximum(other_top, 1.0) / p_new)

    carry = start
    if prepare is not None:
        prepare(0)
    for j in range(NC):
        if prepare is not None and j + 1 < NC:
            prepare(j + 1)
        carry = column(j, carry)
    return carry


def close_sums(state, close, base, sign):
    real = jnp.zeros((8, 2 * W), F32)
    imag = jnp.zeros((8, 2 * W), F32)
    for k in range(NR):
        c = close[base + k]
        b = state[k]
        d = pltpu.roll(c, W, 1)
        for g in range(8):
            part = slice(8 * g, 8 * g + 8)
            real = real - b[part] * c[part] * sign
            imag = imag + b[part] * d[part]
    return jnp.sum(real, keepdims=True), jnp.sum(imag, keepdims=True)


def write_messages(state, board_out, halo_out, peaks, ell, end, sums):
    p, rho_mix, rho = end
    for k in range(NR):
        board_out[pl.ds(k * W, W), :] = state[k]
    board_out[pl.ds(NR * W, 1), :] = p
    board_out[pl.ds(NR * W + 1, 1), :] = rho_mix
    board_out[pl.ds(NR * W + 2, 1), :] = rho
    board_out[pl.ds(NR * W + 3, 1), :] = ell + jnp.sum(jnp.log(peaks[...]), axis=0, keepdims=True)
    board_out[pl.ds(NR * W + 4, 4), :] = jnp.zeros((4, 2 * W), F32)
    halo_out[pl.ds(NC * W + 8, 8), :] = jnp.zeros((8, 2 * W), F32)
    if sums is not None:
        halo_out[pl.ds(NC * W + 8, 1), :] = jnp.broadcast_to(sums[0], (1, 2 * W))
        halo_out[pl.ds(NC * W + 9, 1), :] = jnp.broadcast_to(sums[1], (1, 2 * W))


def places():
    s, q = lax.axis_index("s"), lax.axis_index("q")
    i = jnp.where(s == 0, lax.axis_index("xp"), 1 - lax.axis_index("xp"))
    stays = jnp.logical_or(q == 0, lax.axis_index("c") == 1)
    j = jnp.where(stays, lax.axis_index("yh"), 1 - lax.axis_index("yh"))
    return s, q, 2 * i + j, (1 - q) * NR


def first_kernel(other, lefts_in, rights_in, phases, edge, lefts, rights, board_out, halo_out, state, turned, peaks):
    s, q, _, base = places()
    sign = sign_row()
    one = jnp.ones((1, 2 * W), F32)
    part = 1 - lax.axis_index("c")
    mine = jnp.logical_and(s == 0, q == 0)
    prepare = lambda j: unpack_column(other, j, part, lefts, rights, sign)

    @pl.when(mine)
    def run():
        for k in range(NR):
            state[k] = edge[base + k].astype(F32)
            turned[k] = times_i(state[k], sign)
        end = sweep(
            state, turned, lefts, rights, phases, None, halo_out, peaks, (one, one, one), sign, prepare
        )
        write_messages(state, board_out, halo_out, peaks, 0.0 * one, end, None)

    @pl.when(jnp.logical_not(mine))
    def keep():
        def place(j, unused):
            prepare(j)
            return unused

        lax.fori_loop(0, NC, place, 0)


def load_state(state, turned, edge, board_in, base, s, sign):
    one = jnp.ones((1, 2 * W), F32)
    first = s == 0
    for k in range(NR):
        x = jnp.where(first, edge[base + k].astype(F32), board_in[pl.ds(k * W, W), :])
        state[k] = x
        turned[k] = times_i(x, sign)
    row = lambda n: board_in[pl.ds(NR * W + n, 1), :]
    p = jnp.maximum(jnp.where(first, one, row(0)), 1.0)
    rho_mix = jnp.where(first, one, row(1))
    rho = jnp.where(first, one, row(2))
    ell = jnp.where(first, 0.0 * one, row(3))
    return (p, rho_mix, rho), ell


def second_kernel(phases, edge, lefts, rights, close, board_in, halo_in, board_out, halo_out, state, turned, peaks):
    s, q, _, base = places()

    @pl.when(s != q)
    def run():
        sign = sign_row()
        start, ell = load_state(state, turned, edge, board_in, base, s, sign)
        end = sweep(
            state, turned, lefts, rights, phases, halo_in, halo_out, peaks, start, sign
        )
        sums = close_sums(state, close, base, sign)
        write_messages(state, board_out, halo_out, peaks, ell, end, sums)


def third_kernel(phases, edge, lefts, rights, close, board_in, halo_in, out, state, turned, peaks, halo_out):
    s, q, own, base = places()
    mine = jnp.logical_and(s == 1, q == 1)

    @pl.when(mine)
    def run():
        sign = sign_row()
        start, ell = load_state(state, turned, edge, board_in, base, s, sign)
        p, rho_mix, _ = sweep(
            state, turned, lefts, rights, phases, halo_in, halo_out, peaks, start, sign
        )
        ell = ell + jnp.sum(jnp.log(peaks[...]), axis=0, keepdims=True)
        real, imag = close_sums(state, close, base, sign)
        factor = 1.0 / math.sqrt(2 * NR * W * W)
        real = (real + rho_mix * halo_in[pl.ds(NC * W + 8, 1), :]) / p * factor
        imag = (imag + rho_mix * halo_in[pl.ds(NC * W + 9, 1), :]) / p * factor
        index = 4 * (2 * lax.axis_index("z") + lax.axis_index("c")) + own
        lane = lax.broadcasted_iota(jnp.int32, (1, 2 * W), 1)
        row = jnp.where(lane == index, real, 0.0)
        row = row + jnp.where(lane == index + 32, imag, 0.0)
        row = row + jnp.where(lane == index + 64, ell, 0.0)
        out[...] = row

    @pl.when(jnp.logical_not(mine))
    def nothing():
        out[...] = jnp.zeros((1, 2 * W), F32)


def finish_kernel(blocks, amps, logs, total, top):
    found = jnp.sum(blocks[...], axis=0, keepdims=True)
    real, imag, ell = found, pltpu.roll(found, 96, 1), pltpu.roll(found, 64, 1)
    used = lax.broadcasted_iota(jnp.int32, (1, 2 * W), 1) < 32
    high = jnp.max(jnp.where(used, ell, 0.0), axis=1, keepdims=True)
    weight = jnp.where(used, jnp.exp(jnp.where(used, ell - high, 0.0)), 0.0)
    top[...] = high
    sums = [jnp.sum(x * weight, axis=1, keepdims=True) for x in (real, imag)]
    total[...] = jnp.concatenate(sums, 1)
    at = 4 * (2 * lax.axis_index("z") + lax.axis_index("c"))
    shift = jnp.where(at == 0, 0, 2 * W - at)
    amps[0:1, :] = pltpu.roll(real, shift, 1)[:, 0:4]
    amps[1:2, :] = pltpu.roll(imag, shift, 1)[:, 0:4]
    logs[...] = pltpu.roll(ell, shift, 1)[:, 0:4]


def call(kernel, outs, scratch, args, specs=None, aliases=None):
    return pl.pallas_call(
        kernel,
        out_shape=outs,
        in_specs=specs or [vmem()] * len(args),
        out_specs=jax.tree.map(lambda _: vmem(), outs),
        scratch_shapes=scratch,
        input_output_aliases=aliases or {},
        compiler_params=pltpu.CompilerParams(vmem_limit_bytes=20 * 2**20),
    )(*args)


def shape(*dims, dtype=F32):
    return jax.ShapeDtypeStruct(dims, dtype)


def chip(s, xp, yh, q):
    return 8 * s + 4 * xp + 2 * yh + q


def along_columns(value, q):
    pairs = [(chip(0, xp, yh, q), chip(1, 1 - xp, yh, q)) for xp in range(2) for yh in range(2)]
    return lax.ppermute(value, GRID, pairs)


def along_rows(value, s):
    pairs = []
    for xp in range(2):
        for yh in range(2):
            source = 2 * chip(s, xp, yh, 0)
            pairs.append((source, 2 * chip(s, xp, 1 - yh, 1)))
            pairs.append((source + 1, 2 * chip(s, xp, yh, 1) + 1))
    return lax.ppermute(value, (*GRID, "c"), pairs)


def swapped(value):
    return lax.ppermute(value, "c", [(0, 1), (1, 0)])


def gathered(found):
    count = lax.axis_size(AXES)
    spread = jnp.broadcast_to(found[None], (count, *found.shape))
    return lax.all_to_all(spread, AXES, 0, 0, tiled=True).reshape(count, found.shape[1])


def body(layout, assign, edge, gate_left, gate_right, phase_angle, close):
    cosine, sine = jnp.cos(phase_angle), jnp.sin(phase_angle)
    cosine = jnp.concatenate([cosine, cosine], -1)
    sine = jnp.concatenate([-sine, sine], -1)
    hbm = pl.BlockSpec(memory_space=pltpu.HBM)
    packed = call(
        pack_kernel,
        shape(8, BLOCK, 2 * W),
        [
            pltpu.SMEM((1, 16), jnp.int32),
            pltpu.SMEM((1, 4), jnp.int32),
            pltpu.VMEM(gate_left.shape, BF16),
            pltpu.VMEM(gate_right.shape, BF16),
            pltpu.SemaphoreType.DMA((4,)),
        ],
        [
            pltpu.with_memory_space_constraint(x, pltpu.HBM)
            for x in (layout.T, assign.T, gate_left, gate_right)
        ],
        [hbm, hbm, hbm, hbm],
    )
    mine = lax.all_to_all(packed, ("xp", "yh", "q"), 0, 0, tiled=True)
    other = swapped(mine)
    state = pltpu.VMEM((NR, W, 2 * W), F32)
    peaks = pltpu.VMEM((NC, 2 * W), F32)
    gates = (shape(NC, NR, W, 2 * W, dtype=BF16), shape(NC, NR, 2 * W, 2 * W, dtype=BF16))
    lefts, rights, phases = call(
        unpack_kernel, (*gates, shape(2 * NC, 2 * W)), [], (mine, cosine, sine)
    )
    lefts, rights, board, halo = call(
        first_kernel,
        (*gates, shape(BOARD, 2 * W), shape(HALO, 2 * W)),
        [state, state, peaks],
        (other, lefts, rights, phases, edge),
        aliases={1: 0, 2: 1},
    )
    board = along_columns(board, 0)
    halo = along_rows(halo, 0)
    board, halo = call(
        second_kernel,
        (shape(BOARD, 2 * W), shape(HALO, 2 * W)),
        [state, state, peaks],
        (phases, edge, lefts, rights, close, board, halo),
    )
    board, halo = along_columns(board, 1), along_rows(halo, 1)
    found = call(
        third_kernel,
        shape(1, 2 * W),
        [state, state, peaks, pltpu.VMEM((HALO, 2 * W), F32)],
        (phases, edge, lefts, rights, close, board, halo),
    )
    amps, logs, total_amp, top_log = call(
        finish_kernel,
        (shape(2, 4), shape(1, 4), shape(1, 2), shape(1, 1)),
        [],
        (gathered(found),),
    )
    return (amps.T, logs.reshape(4), total_amp.reshape(2), top_log.reshape(()))


def solution(mesh):
    split = Mesh(mesh.devices.reshape(2, 2, 2, 2, 4, 2), AXES)
    placed = (
        P(None, GRID),
        P(("z", "c"), GRID),
        P(),
        P(GRID, None, None, None),
        P(GRID, None, None, None),
        P(),
        P(),
    )
    return jax.shard_map(
        body,
        mesh=split,
        in_specs=placed,
        out_specs=(P(("z", "c"), None), P(("z", "c")), P(), P()),
        check_vma=False,
    )
```

```python
import math

import jax
import jax.numpy as jnp
from jax import lax
from jax.experimental import pallas as pl
from jax.experimental.pallas import tpu as pltpu
from jax.sharding import Mesh
from jax.sharding import PartitionSpec as P

AXES = ("s", "xp", "yh", "q", "z", "c")
GRID = ("s", "xp", "yh", "q")
NC = 8
NR = 8
W = 64
BLOCK = 4 * 2 * W + 8
BOARD = NR * W + 8
HALO = NC * W + 16
F32 = jnp.float32
BF16 = jnp.bfloat16


def vmem():
    return pl.BlockSpec(memory_space=pltpu.VMEM)


def sign_row():
    lane = lax.broadcasted_iota(jnp.int32, (1, 2 * W), 1)
    return jnp.where(lane < W, -1.0, 1.0).astype(F32)


def times_i(x, sign):
    return pltpu.roll(x, W, 1) * sign


def pack_kernel(layout_hbm, assign_hbm, left_hbm, right_hbm, out, layout, assign, left, right, sems):
    core = lax.axis_index("c")
    copies = [
        pltpu.make_async_copy(layout_hbm, layout, sems.at[0]),
        pltpu.make_async_copy(assign_hbm, assign, sems.at[1]),
        pltpu.make_async_copy(left_hbm, left, sems.at[2]),
        pltpu.make_async_copy(right_hbm, right, sems.at[3]),
    ]
    for copy in copies:
        copy.start()
    for dest in range(8):
        out[dest, pl.ds(8 * W + 4, 4), :] = jnp.zeros((4, 2 * W), F32)
    for copy in copies:
        copy.wait()
    for t in range(4):
        row = jnp.full((1, 2 * W), assign[0, t].astype(F32), F32)
        for dest in range(8):
            out[dest, pl.ds(8 * W + t, 1), :] = row
    for half in range(2):
        for k in range(4):
            kind = layout[0, (1 - half) * NR + 4 * core + k]
            for n, table in ((2 * k, left), (2 * k + 1, right)):
                x = table[0, kind].astype(F32)
                for dest in range(half, 8, 2):
                    out[dest, pl.ds(W * n, W), :] = x


def unpack_column(source, j, part, lefts, rights, sign):
    for k in range(4):
        row = 4 * part + k
        lefts[j, row] = source[j, pl.ds(2 * W * k, W), :].astype(BF16)
        r = source[j, pl.ds(2 * W * k + W, W), :]
        rights[j, row, pl.ds(0, W), :] = r.astype(BF16)
        rights[j, row, pl.ds(W, W), :] = times_i(r, sign).astype(BF16)


def unpack_kernel(mine, cosine, sine, lefts, rights, phases):
    s, q, own, base = places()
    part, sign = lax.axis_index("c"), sign_row()

    def place(j, unused):
        unpack_column(mine, j, part, lefts, rights, sign)
        return unused

    lax.fori_loop(0, NC, place, 0)
    for j in range(NC):
        value = mine[j, pl.ds(8 * W + own, 1), :]
        for n, table in ((0, cosine), (NC, sine)):
            row = jnp.zeros((1, 2 * W), F32)
            for v in range(4):
                row = jnp.where(value == float(v), table[pl.ds(v, 1), :], row)
            phases[pl.ds(n + j, 1), :] = row


def halves(x):
    high = x.astype(BF16)
    return high, (x - high.astype(F32)).astype(BF16)


def sweep(state, turned, lefts, rights, phases, halo_in, halo_out, peaks, start, sign, prepare=None):
    def column(j, carry):
        p, rho_mix, rho = carry
        scale = 1.0 / p
        cos_row = phases[pl.ds(j, 1), :] * scale
        sin_row = phases[pl.ds(NC + j, 1), :] * scale
        cos_turn = cos_row * sign
        sin_turn = sin_row * sign
        boards = [state[k] for k in range(NR)]
        turns = [turned[k] for k in range(NR)]
        halo_out[pl.ds(j * W, W), :] = boards[0]
        if halo_in is None:
            below = below_turn = None
        else:
            below = halo_in[pl.ds(j * W, W), :] * rho_mix
            below_turn = times_i(below, sign)
        top = jnp.zeros((8, 2 * W), F32)
        for k in range(NR):
            after = boards[k + 1] if k + 1 < NR else below
            mixed = boards[k] if after is None else boards[k] + 0.5 * after
            after = turns[k + 1] if k + 1 < NR else below_turn
            turn = turns[k] if after is None else turns[k] + 0.5 * after
            mh, ml = halves(mixed)
            th, tl = halves(turn)
            both = jnp.dot(
                lefts[j, k],
                jnp.concatenate([jnp.concatenate([mh, th], 0), jnp.concatenate([ml, tl], 0)], 1),
                preferred_element_type=F32,
            )
            middle = both[:, : 2 * W] + both[:, 2 * W :]
            dh, dl = halves(middle)
            two = jnp.dot(
                jnp.concatenate([dh, dl], 0), rights[j, k], preferred_element_type=F32
            )
            plain = two[:W] + two[W:]
            flip = pltpu.roll(plain, W, 1)
            out = plain * cos_row + flip * sin_row
            state[k] = out
            turned[k] = flip * cos_turn - plain * sin_turn
            for g in range(8):
                top = jnp.maximum(top, jnp.abs(out[8 * g : 8 * g + 8]))
        own_top = jnp.broadcast_to(jnp.max(top, keepdims=True), (1, 2 * W))
        halo_out[pl.ds(NC * W + j, 1), :] = own_top
        if halo_in is None:
            other_top = jnp.zeros((1, 2 * W), F32)
        else:
            other_top = halo_in[pl.ds(NC * W + j, 1), :]
        p_new = jnp.maximum(jnp.maximum(own_top, other_top * rho), 1.0)
        peaks[pl.ds(j, 1), :] = p_new
        return (p_new, rho, rho * jnp.maximum(other_top, 1.0) / p_new)

    carry = start
    if prepare is not None:
        prepare(0)
    for j in range(NC):
        if prepare is not None and j + 1 < NC:
            prepare(j + 1)
        carry = column(j, carry)
    return carry


def close_sums(state, close, base, sign):
    real = jnp.zeros((8, 2 * W), F32)
    imag = jnp.zeros((8, 2 * W), F32)
    for k in range(NR):
        c = close[base + k]
        b = state[k]
        d = pltpu.roll(c, W, 1)
        for g in range(8):
            part = slice(8 * g, 8 * g + 8)
            real = real - b[part] * c[part] * sign
            imag = imag + b[part] * d[part]
    return jnp.sum(real, keepdims=True), jnp.sum(imag, keepdims=True)


def write_messages(state, board_out, halo_out, peaks, ell, end, sums):
    p, rho_mix, rho = end
    for k in range(NR):
        board_out[pl.ds(k * W, W), :] = state[k]
    board_out[pl.ds(NR * W, 1), :] = p
    board_out[pl.ds(NR * W + 1, 1), :] = rho_mix
    board_out[pl.ds(NR * W + 2, 1), :] = rho
    board_out[pl.ds(NR * W + 3, 1), :] = ell + jnp.sum(jnp.log(peaks[...]), axis=0, keepdims=True)
    board_out[pl.ds(NR * W + 4, 4), :] = jnp.zeros((4, 2 * W), F32)
    halo_out[pl.ds(NC * W + 8, 8), :] = jnp.zeros((8, 2 * W), F32)
    if sums is not None:
        halo_out[pl.ds(NC * W + 8, 1), :] = jnp.broadcast_to(sums[0], (1, 2 * W))
        halo_out[pl.ds(NC * W + 9, 1), :] = jnp.broadcast_to(sums[1], (1, 2 * W))


def places():
    s, q = lax.axis_index("s"), lax.axis_index("q")
    i = jnp.where(s == 0, lax.axis_index("xp"), 1 - lax.axis_index("xp"))
    stays = jnp.logical_or(q == 0, lax.axis_index("c") == 1)
    j = jnp.where(stays, lax.axis_index("yh"), 1 - lax.axis_index("yh"))
    return s, q, 2 * i + j, (1 - q) * NR


def first_kernel(other, lefts_in, rights_in, phases, edge, lefts, rights, board_out, halo_out, state, turned, peaks):
    s, q, own, base = places()
    sign = sign_row()
    one = jnp.ones((1, 2 * W), F32)
    part = 1 - lax.axis_index("c")
    mine = jnp.logical_and(s == 0, q == 0)
    prepare = lambda j: unpack_column(other, j, part, lefts, rights, sign)

    @pl.when(mine)
    def run():
        for k in range(NR):
            state[k] = edge[base + k].astype(F32)
            turned[k] = times_i(state[k], sign)
        end = sweep(
            state, turned, lefts, rights, phases, None, halo_out, peaks, (one, one, one), sign, prepare
        )
        write_messages(state, board_out, halo_out, peaks, 0.0 * one, end, None)

    @pl.when(jnp.logical_not(mine))
    def keep():
        def place(j, unused):
            prepare(j)
            return unused

        lax.fori_loop(0, NC, place, 0)


def load_state(state, turned, edge, board_in, base, s, sign):
    one = jnp.ones((1, 2 * W), F32)
    first = s == 0
    for k in range(NR):
        x = jnp.where(first, edge[base + k].astype(F32), board_in[pl.ds(k * W, W), :])
        state[k] = x
        turned[k] = times_i(x, sign)
    row = lambda n: board_in[pl.ds(NR * W + n, 1), :]
    p = jnp.maximum(jnp.where(first, one, row(0)), 1.0)
    rho_mix = jnp.where(first, one, row(1))
    rho = jnp.where(first, one, row(2))
    ell = jnp.where(first, 0.0 * one, row(3))
    return (p, rho_mix, rho), ell


def second_kernel(phases, edge, lefts, rights, close, board_in, halo_in, board_out, halo_out, state, turned, peaks):
    s, q, own, base = places()

    @pl.when(s != q)
    def run():
        sign = sign_row()
        start, ell = load_state(state, turned, edge, board_in, base, s, sign)
        end = sweep(
            state, turned, lefts, rights, phases, halo_in, halo_out, peaks, start, sign
        )
        sums = close_sums(state, close, base, sign)
        write_messages(state, board_out, halo_out, peaks, ell, end, sums)


def third_kernel(phases, edge, lefts, rights, close, board_in, halo_in, out, state, turned, peaks, halo_out):
    s, q, own, base = places()
    mine = jnp.logical_and(s == 1, q == 1)

    @pl.when(mine)
    def run():
        sign = sign_row()
        start, ell = load_state(state, turned, edge, board_in, base, s, sign)
        p, rho_mix, rho = sweep(
            state, turned, lefts, rights, phases, halo_in, halo_out, peaks, start, sign
        )
        ell = ell + jnp.sum(jnp.log(peaks[...]), axis=0, keepdims=True)
        real, imag = close_sums(state, close, base, sign)
        factor = 1.0 / math.sqrt(2 * NR * W * W)
        real = (real + rho_mix * halo_in[pl.ds(NC * W + 8, 1), :]) / p * factor
        imag = (imag + rho_mix * halo_in[pl.ds(NC * W + 9, 1), :]) / p * factor
        index = 4 * (2 * lax.axis_index("z") + lax.axis_index("c")) + own
        lane = lax.broadcasted_iota(jnp.int32, (1, 2 * W), 1)
        row = jnp.where(lane == index, real, 0.0)
        row = row + jnp.where(lane == index + 32, imag, 0.0)
        row = row + jnp.where(lane == index + 64, ell, 0.0)
        out[...] = row

    @pl.when(jnp.logical_not(mine))
    def nothing():
        out[...] = jnp.zeros((1, 2 * W), F32)


def finish_kernel(blocks, amps, logs, total, top):
    found = jnp.sum(blocks[...], axis=0, keepdims=True)
    real, imag, ell = found, pltpu.roll(found, 96, 1), pltpu.roll(found, 64, 1)
    used = lax.broadcasted_iota(jnp.int32, (1, 2 * W), 1) < 32
    high = jnp.max(jnp.where(used, ell, 0.0), axis=1, keepdims=True)
    weight = jnp.where(used, jnp.exp(jnp.where(used, ell - high, 0.0)), 0.0)
    top[...] = high
    sums = [jnp.sum(x * weight, axis=1, keepdims=True) for x in (real, imag)]
    total[...] = jnp.concatenate(sums, 1)
    at = 4 * (2 * lax.axis_index("z") + lax.axis_index("c"))
    shift = jnp.where(at == 0, 0, 2 * W - at)
    amps[0:1, :] = pltpu.roll(real, shift, 1)[:, 0:4]
    amps[1:2, :] = pltpu.roll(imag, shift, 1)[:, 0:4]
    logs[...] = pltpu.roll(ell, shift, 1)[:, 0:4]


def call(kernel, outs, scratch, args, specs=None, aliases=None):
    return pl.pallas_call(
        kernel,
        out_shape=outs,
        in_specs=specs or [vmem()] * len(args),
        out_specs=jax.tree.map(lambda _: vmem(), outs),
        scratch_shapes=scratch,
        input_output_aliases=aliases or {},
        compiler_params=pltpu.CompilerParams(vmem_limit_bytes=20 * 2**20),
    )(*args)


def shape(*dims, dtype=F32):
    return jax.ShapeDtypeStruct(dims, dtype)


def chip(s, xp, yh, q):
    return 8 * s + 4 * xp + 2 * yh + q


def along_columns(value, q):
    pairs = [(chip(0, xp, yh, q), chip(1, 1 - xp, yh, q)) for xp in range(2) for yh in range(2)]
    return lax.ppermute(value, GRID, pairs)


def along_rows(value, s):
    pairs = []
    for xp in range(2):
        for yh in range(2):
            source = 2 * chip(s, xp, yh, 0)
            pairs.append((source, 2 * chip(s, xp, 1 - yh, 1)))
            pairs.append((source + 1, 2 * chip(s, xp, yh, 1) + 1))
    return lax.ppermute(value, (*GRID, "c"), pairs)


def swapped(value):
    return lax.ppermute(value, "c", [(0, 1), (1, 0)])


def gathered(found):
    count = lax.axis_size(AXES)
    spread = jnp.broadcast_to(found[None], (count, *found.shape))
    return lax.all_to_all(spread, AXES, 0, 0, tiled=True).reshape(count, found.shape[1])


def body(layout, assign, edge, gate_left, gate_right, phase_angle, close):
    cosine, sine = jnp.cos(phase_angle), jnp.sin(phase_angle)
    cosine = jnp.concatenate([cosine, cosine], -1)
    sine = jnp.concatenate([-sine, sine], -1)
    hbm = pl.BlockSpec(memory_space=pltpu.HBM)
    packed = call(
        pack_kernel,
        shape(8, BLOCK, 2 * W),
        [
            pltpu.SMEM((1, 16), jnp.int32),
            pltpu.SMEM((1, 4), jnp.int32),
            pltpu.VMEM(gate_left.shape, BF16),
            pltpu.VMEM(gate_right.shape, BF16),
            pltpu.SemaphoreType.DMA((4,)),
        ],
        [
            pltpu.with_memory_space_constraint(x, pltpu.HBM)
            for x in (layout.T, assign.T, gate_left, gate_right)
        ],
        [hbm, hbm, hbm, hbm],
    )
    mine = lax.all_to_all(packed, ("xp", "yh", "q"), 0, 0, tiled=True)
    other = swapped(mine)
    state = pltpu.VMEM((NR, W, 2 * W), F32)
    peaks = pltpu.VMEM((NC, 2 * W), F32)
    gates = (shape(NC, NR, W, 2 * W, dtype=BF16), shape(NC, NR, 2 * W, 2 * W, dtype=BF16))
    lefts, rights, phases = call(
        unpack_kernel, (*gates, shape(2 * NC, 2 * W)), [], (mine, cosine, sine)
    )
    lefts, rights, board, halo = call(
        first_kernel,
        (*gates, shape(BOARD, 2 * W), shape(HALO, 2 * W)),
        [state, state, peaks],
        (other, lefts, rights, phases, edge),
        aliases={1: 0, 2: 1},
    )
    board, halo = along_columns(board, 0), along_rows(halo, 0)
    board, halo = call(
        second_kernel,
        (shape(BOARD, 2 * W), shape(HALO, 2 * W)),
        [state, state, peaks],
        (phases, edge, lefts, rights, close, board, halo),
    )
    board, halo = along_columns(board, 1), along_rows(halo, 1)
    found = call(
        third_kernel,
        shape(1, 2 * W),
        [state, state, peaks, pltpu.VMEM((HALO, 2 * W), F32)],
        (phases, edge, lefts, rights, close, board, halo),
    )
    amps, logs, total_amp, top_log = call(
        finish_kernel,
        (shape(2, 4), shape(1, 4), shape(1, 2), shape(1, 1)),
        [],
        (gathered(found),),
    )
    return (amps.T, logs.reshape(4), total_amp.reshape(2), top_log.reshape(()))


def solution(mesh):
    split = Mesh(mesh.devices.reshape(2, 2, 2, 2, 4, 2), AXES)
    placed = (
        P(None, GRID),
        P(("z", "c"), GRID),
        P(),
        P(GRID, None, None, None),
        P(GRID, None, None, None),
        P(),
        P(),
    )
    return jax.shard_map(
        body,
        mesh=split,
        in_specs=placed,
        out_specs=(P(("z", "c"), None), P(("z", "c")), P(), P()),
        check_vma=False,
    )
```

```python
import math

import jax
import jax.numpy as jnp
from jax import lax
from jax.experimental import pallas as pl
from jax.experimental.pallas import tpu as pltpu
from jax.sharding import Mesh
from jax.sharding import PartitionSpec as P

AXES = ("s", "xp", "yh", "q", "z", "c")
GRID = ("s", "xp", "yh", "q")
NC = 8
NR = 8
W = 64
BLOCK = 4 * 2 * W + 8
BOARD = NR * W + 8
HALO = NC * W + 24
F32 = jnp.float32
BF16 = jnp.bfloat16


def vmem():
    return pl.BlockSpec(memory_space=pltpu.VMEM)


def sign_row():
    lane = lax.broadcasted_iota(jnp.int32, (1, 2 * W), 1)
    return jnp.where(lane < W, -1.0, 1.0).astype(F32)


def times_i(x, sign):
    return pltpu.roll(x, W, 1) * sign


def pack_kernel(layout_hbm, assign_hbm, left_hbm, right_hbm, out, layout, assign, left, right, sems):
    core = lax.axis_index("c")
    copies = [
        pltpu.make_async_copy(layout_hbm, layout, sems.at[0]),
        pltpu.make_async_copy(assign_hbm, assign, sems.at[1]),
        pltpu.make_async_copy(left_hbm, left, sems.at[2]),
        pltpu.make_async_copy(right_hbm, right, sems.at[3]),
    ]
    for copy in copies:
        copy.start()
    for dest in range(8):
        out[dest, pl.ds(8 * W + 4, 4), :] = jnp.zeros((4, 2 * W), F32)
    for copy in copies:
        copy.wait()
    for t in range(4):
        row = jnp.full((1, 2 * W), assign[0, t].astype(F32), F32)
        for dest in range(8):
            out[dest, pl.ds(8 * W + t, 1), :] = row
    for half in range(2):
        for k in range(4):
            kind = layout[0, (1 - half) * NR + 4 * core + k]
            for n, table in ((2 * k, left), (2 * k + 1, right)):
                x = table[0, kind].astype(F32)
                for dest in range(half, 8, 2):
                    out[dest, pl.ds(W * n, W), :] = x


def unpack_column(source, j, part, lefts, rights, sign):
    for k in range(4):
        row = 4 * part + k
        lefts[j, row] = source[j, pl.ds(2 * W * k, W), :].astype(BF16)
        r = source[j, pl.ds(2 * W * k + W, W), :]
        rights[j, row, pl.ds(0, W), :] = r.astype(BF16)
        rights[j, row, pl.ds(W, W), :] = times_i(r, sign).astype(BF16)


def unpack_kernel(mine, cosine, sine, lefts, rights, phases):
    _, _, own, _ = places()
    part, sign = lax.axis_index("c"), sign_row()

    def place(j, unused):
        unpack_column(mine, j, part, lefts, rights, sign)
        return unused

    lax.fori_loop(0, NC, place, 0)
    for j in range(NC):
        value = mine[j, pl.ds(8 * W + own, 1), :]
        for n, table in ((0, cosine), (NC, sine)):
            row = jnp.zeros((1, 2 * W), F32)
            for v in range(4):
                row = jnp.where(value == float(v), table[pl.ds(v, 1), :], row)
            phases[pl.ds(n + j, 1), :] = row


def halves(x):
    high = x.astype(BF16)
    return high, (x - high.astype(F32)).astype(BF16)


def sweep(state, turned, lefts, rights, phases, halo_in, halo_out, peaks, start, sign, prepare=None):
    def column(j, carry):
        p, rho_mix, rho = carry
        scale = 1.0 / p
        cos_row = phases[pl.ds(j, 1), :] * scale
        sin_row = phases[pl.ds(NC + j, 1), :] * scale
        cos_turn = cos_row * sign
        sin_turn = sin_row * sign
        boards = [state[k] for k in range(NR)]
        turns = [turned[k] for k in range(NR)]
        halo_out[pl.ds(j * W, W), :] = boards[0]
        if halo_in is None:
            below = below_turn = None
        else:
            below = halo_in[pl.ds(j * W, W), :] * (rho_mix * 0.5**NR)
            below_turn = times_i(below, sign)
        top = jnp.zeros((8, 2 * W), F32)
        for k in range(NR):
            after = boards[k + 1] if k + 1 < NR else below
            mixed = boards[k] if after is None else boards[k] + after
            after = turns[k + 1] if k + 1 < NR else below_turn
            turn = turns[k] if after is None else turns[k] + after
            mh, ml = halves(mixed)
            th, tl = halves(turn)
            both = jnp.dot(
                lefts[j, k],
                jnp.concatenate([jnp.concatenate([mh, th], 0), jnp.concatenate([ml, tl], 0)], 1),
                preferred_element_type=F32,
            )
            middle = both[:, : 2 * W] + both[:, 2 * W :]
            dh, dl = halves(middle)
            two = jnp.dot(
                jnp.concatenate([dh, dl], 0), rights[j, k], preferred_element_type=F32
            )
            plain = two[:W] + two[W:]
            flip = pltpu.roll(plain, W, 1)
            out = plain * cos_row + flip * sin_row
            state[k] = out
            turned[k] = flip * cos_turn - plain * sin_turn
            row_top = jnp.abs(out[0:8])
            for g in range(1, 8):
                row_top = jnp.maximum(row_top, jnp.abs(out[8 * g : 8 * g + 8]))
            top = jnp.maximum(top, row_top * 2.0**k)
        own_top = jnp.broadcast_to(jnp.max(top, keepdims=True), (1, 2 * W))
        halo_out[pl.ds(NC * W + j, 1), :] = own_top
        if halo_in is None:
            other_top = jnp.zeros((1, 2 * W), F32)
        else:
            other_top = halo_in[pl.ds(NC * W + j, 1), :]
        p_new = jnp.maximum(jnp.maximum(own_top, other_top * rho), 1.0)
        peaks[pl.ds(j, 1), :] = p_new
        return (p_new, rho, rho * jnp.maximum(other_top, 1.0) / p_new)

    carry = start
    if prepare is not None:
        prepare(0)
    for j in range(NC):
        if prepare is not None and j + 1 < NC:
            prepare(j + 1)
        carry = column(j, carry)
    return carry


def close_sums(state, close, base, sign):
    real = jnp.zeros((8, 2 * W), F32)
    imag = jnp.zeros((8, 2 * W), F32)
    for k in range(NR):
        c = close[base + k]
        b = state[k]
        d = pltpu.roll(c, W, 1)
        row_real = b[0:8] * c[0:8]
        row_imag = b[0:8] * d[0:8]
        for g in range(1, 8):
            part = slice(8 * g, 8 * g + 8)
            row_real = row_real + b[part] * c[part]
            row_imag = row_imag + b[part] * d[part]
        real = real + row_real * 2.0**k
        imag = imag + row_imag * 2.0**k
    return -real * sign, imag


def write_messages(state, board_out, halo_out, peaks, ell, end, sums):
    p, rho_mix, rho = end
    for k in range(NR):
        board_out[pl.ds(k * W, W), :] = state[k]
    board_out[pl.ds(NR * W, 1), :] = p
    board_out[pl.ds(NR * W + 1, 1), :] = rho_mix
    board_out[pl.ds(NR * W + 2, 1), :] = rho
    board_out[pl.ds(NR * W + 3, 1), :] = ell + jnp.sum(jnp.log(peaks[...]), axis=0, keepdims=True)
    board_out[pl.ds(NR * W + 4, 4), :] = jnp.zeros((4, 2 * W), F32)
    if sums is not None:
        halo_out[pl.ds(NC * W + 8, 8), :] = sums[0]
        halo_out[pl.ds(NC * W + 16, 8), :] = sums[1]


def places():
    s, q = lax.axis_index("s"), lax.axis_index("q")
    i = jnp.where(s == 0, lax.axis_index("xp"), 1 - lax.axis_index("xp"))
    stays = jnp.logical_or(q == 0, lax.axis_index("c") == 1)
    j = jnp.where(stays, lax.axis_index("yh"), 1 - lax.axis_index("yh"))
    return s, q, 2 * i + j, (1 - q) * NR


def first_kernel(other, lefts_in, rights_in, phases, edge, lefts, rights, board_out, halo_out, state, turned, peaks):
    s, q, _, base = places()
    sign = sign_row()
    one = jnp.ones((1, 2 * W), F32)
    part = 1 - lax.axis_index("c")
    mine = jnp.logical_and(s == 0, q == 0)
    prepare = lambda j: unpack_column(other, j, part, lefts, rights, sign)

    @pl.when(mine)
    def run():
        for k in range(NR):
            x = edge[base + k].astype(F32) * 0.5**k
            state[k] = x
            turned[k] = times_i(x, sign)
        end = sweep(
            state, turned, lefts, rights, phases, None, halo_out, peaks, (one, one, one), sign, prepare
        )
        write_messages(state, board_out, halo_out, peaks, 0.0 * one, end, None)

    @pl.when(jnp.logical_not(mine))
    def keep():
        def place(j, unused):
            prepare(j)
            return unused

        lax.fori_loop(0, NC, place, 0)


def load_state(state, turned, edge, board_in, base, s, sign):
    one = jnp.ones((1, 2 * W), F32)
    first = s == 0
    for k in range(NR):
        x = jnp.where(first, edge[base + k].astype(F32) * 0.5**k, board_in[pl.ds(k * W, W), :])
        state[k] = x
        turned[k] = times_i(x, sign)
    row = lambda n: board_in[pl.ds(NR * W + n, 1), :]
    p = jnp.maximum(jnp.where(first, one, row(0)), 1.0)
    rho_mix = jnp.where(first, one, row(1))
    rho = jnp.where(first, one, row(2))
    ell = jnp.where(first, 0.0 * one, row(3))
    return (p, rho_mix, rho), ell


def second_kernel(phases, edge, lefts, rights, close, board_in, halo_in, board_out, halo_out, state, turned, peaks):
    s, q, _, base = places()

    @pl.when(s != q)
    def run():
        sign = sign_row()
        start, ell = load_state(state, turned, edge, board_in, base, s, sign)
        end = sweep(
            state, turned, lefts, rights, phases, halo_in, halo_out, peaks, start, sign
        )
        sums = close_sums(state, close, base, sign)
        write_messages(state, board_out, halo_out, peaks, ell, end, sums)


def third_kernel(phases, edge, lefts, rights, close, board_in, halo_in, out, state, turned, peaks, halo_out):
    s, q, own, base = places()
    mine = jnp.logical_and(s == 1, q == 1)

    @pl.when(mine)
    def run():
        sign = sign_row()
        start, ell = load_state(state, turned, edge, board_in, base, s, sign)
        p, rho_mix, _ = sweep(
            state, turned, lefts, rights, phases, halo_in, halo_out, peaks, start, sign
        )
        ell = ell + jnp.sum(jnp.log(peaks[...]), axis=0, keepdims=True)
        real, imag = close_sums(state, close, base, sign)
        factor = 1.0 / math.sqrt(2 * NR * W * W)
        scale = factor / p
        real = real + rho_mix * halo_in[pl.ds(NC * W + 8, 8), :]
        imag = imag + rho_mix * halo_in[pl.ds(NC * W + 16, 8), :]
        real = jnp.sum(real, keepdims=True) * scale
        imag = jnp.sum(imag, keepdims=True) * scale
        index = 4 * (2 * lax.axis_index("z") + lax.axis_index("c")) + own
        lane = lax.broadcasted_iota(jnp.int32, (1, 2 * W), 1)
        row = jnp.where(lane == index, real, 0.0)
        row = row + jnp.where(lane == index + 32, imag, 0.0)
        row = row + jnp.where(lane == index + 64, ell, 0.0)
        out[...] = row

    @pl.when(jnp.logical_not(mine))
    def nothing():
        out[...] = jnp.zeros((1, 2 * W), F32)


def finish_kernel(blocks, amps, logs, total, top):
    found = jnp.sum(blocks[...], axis=0, keepdims=True)
    real, imag, ell = found, pltpu.roll(found, 96, 1), pltpu.roll(found, 64, 1)
    used = lax.broadcasted_iota(jnp.int32, (1, 2 * W), 1) < 32
    high = jnp.max(jnp.where(used, ell, 0.0), axis=1, keepdims=True)
    weight = jnp.where(used, jnp.exp(jnp.where(used, ell - high, 0.0)), 0.0)
    top[...] = high
    sums = [jnp.sum(x * weight, axis=1, keepdims=True) for x in (real, imag)]
    total[...] = jnp.concatenate(sums, 1)
    at = 4 * (2 * lax.axis_index("z") + lax.axis_index("c"))
    shift = jnp.where(at == 0, 0, 2 * W - at)
    amps[0:1, :] = pltpu.roll(real, shift, 1)[:, 0:4]
    amps[1:2, :] = pltpu.roll(imag, shift, 1)[:, 0:4]
    logs[...] = pltpu.roll(ell, shift, 1)[:, 0:4]


def call(kernel, outs, scratch, args, specs=None, aliases=None):
    return pl.pallas_call(
        kernel,
        out_shape=outs,
        in_specs=specs or [vmem()] * len(args),
        out_specs=jax.tree.map(lambda _: vmem(), outs),
        scratch_shapes=scratch,
        input_output_aliases=aliases or {},
        compiler_params=pltpu.CompilerParams(vmem_limit_bytes=20 * 2**20),
    )(*args)


def shape(*dims, dtype=F32):
    return jax.ShapeDtypeStruct(dims, dtype)


def chip(s, xp, yh, q):
    return 8 * s + 4 * xp + 2 * yh + q


def along_columns(value, q):
    pairs = [(chip(0, xp, yh, q), chip(1, 1 - xp, yh, q)) for xp in range(2) for yh in range(2)]
    return lax.ppermute(value, GRID, pairs)


def along_rows(value, s):
    pairs = []
    for xp in range(2):
        for yh in range(2):
            source = 2 * chip(s, xp, yh, 0)
            pairs.append((source, 2 * chip(s, xp, 1 - yh, 1)))
            pairs.append((source + 1, 2 * chip(s, xp, yh, 1) + 1))
    return lax.ppermute(value, (*GRID, "c"), pairs)


def swapped(value):
    return lax.ppermute(value, "c", [(0, 1), (1, 0)])


def gathered(found):
    count = lax.axis_size(AXES)
    spread = jnp.broadcast_to(found[None], (count, *found.shape))
    return lax.all_to_all(spread, AXES, 0, 0, tiled=True).reshape(count, found.shape[1])


def body(layout, assign, edge, gate_left, gate_right, phase_angle, close):
    cosine, sine = jnp.cos(phase_angle), jnp.sin(phase_angle)
    cosine = jnp.concatenate([cosine, cosine], -1)
    sine = jnp.concatenate([-sine, sine], -1)
    hbm = pl.BlockSpec(memory_space=pltpu.HBM)
    packed = call(
        pack_kernel,
        shape(8, BLOCK, 2 * W),
        [
            pltpu.SMEM((1, 16), jnp.int32),
            pltpu.SMEM((1, 4), jnp.int32),
            pltpu.VMEM(gate_left.shape, BF16),
            pltpu.VMEM(gate_right.shape, BF16),
            pltpu.SemaphoreType.DMA((4,)),
        ],
        [
            pltpu.with_memory_space_constraint(x, pltpu.HBM)
            for x in (layout.T, assign.T, gate_left, gate_right)
        ],
        [hbm, hbm, hbm, hbm],
    )
    mine = lax.all_to_all(packed, ("xp", "yh", "q"), 0, 0, tiled=True)
    other = swapped(mine)
    state = pltpu.VMEM((NR, W, 2 * W), F32)
    peaks = pltpu.VMEM((NC, 2 * W), F32)
    gates = (shape(NC, NR, W, 2 * W, dtype=BF16), shape(NC, NR, 2 * W, 2 * W, dtype=BF16))
    lefts, rights, phases = call(
        unpack_kernel, (*gates, shape(2 * NC, 2 * W)), [], (mine, cosine, sine)
    )
    lefts, rights, board, halo = call(
        first_kernel,
        (*gates, shape(BOARD, 2 * W), shape(HALO, 2 * W)),
        [state, state, peaks],
        (other, lefts, rights, phases, edge),
        aliases={1: 0, 2: 1},
    )
    board = along_columns(board, 0)
    halo = along_rows(halo, 0)
    board, halo = call(
        second_kernel,
        (shape(BOARD, 2 * W), shape(HALO, 2 * W)),
        [state, state, peaks],
        (phases, edge, lefts, rights, close, board, halo),
    )
    board, halo = along_columns(board, 1), along_rows(halo, 1)
    found = call(
        third_kernel,
        shape(1, 2 * W),
        [state, state, peaks, pltpu.VMEM((HALO, 2 * W), F32)],
        (phases, edge, lefts, rights, close, board, halo),
    )
    amps, logs, total_amp, top_log = call(
        finish_kernel,
        (shape(2, 4), shape(1, 4), shape(1, 2), shape(1, 1)),
        [],
        (gathered(found),),
    )
    return (amps.T, logs.reshape(4), total_amp.reshape(2), top_log.reshape(()))


def solution(mesh):
    split = Mesh(mesh.devices.reshape(2, 2, 2, 2, 4, 2), AXES)
    placed = (
        P(None, GRID),
        P(("z", "c"), GRID),
        P(),
        P(GRID, None, None, None),
        P(GRID, None, None, None),
        P(),
        P(),
    )
    return jax.shard_map(
        body,
        mesh=split,
        in_specs=placed,
        out_specs=(P(("z", "c"), None), P(("z", "c")), P(), P()),
        check_vma=False,
    )
```

```python
import math

import jax
import jax.numpy as jnp
from jax import lax
from jax.experimental import pallas as pl
from jax.experimental.pallas import tpu as pltpu
from jax.sharding import Mesh
from jax.sharding import PartitionSpec as P

AXES = ("s", "xp", "yh", "q", "z", "c")
GRID = ("s", "xp", "yh", "q")
NC = 8
NR = 8
W = 64
BLOCK = 4 * 2 * W + 8
BOARD = NR * W + 8
HALO = NC * W + 24
FIRST = (NC - 1) * W + 8
F32 = jnp.float32
BF16 = jnp.bfloat16


def vmem():
    return pl.BlockSpec(memory_space=pltpu.VMEM)


def sign_row():
    lane = lax.broadcasted_iota(jnp.int32, (1, 2 * W), 1)
    return jnp.where(lane < W, -1.0, 1.0).astype(F32)


def times_i(x, sign):
    return pltpu.roll(x, W, 1) * sign


def pack_kernel(layout_hbm, assign_hbm, left_hbm, right_hbm, out, layout, assign, left, right, sems):
    core = lax.axis_index("c")
    copies = [
        pltpu.make_async_copy(layout_hbm, layout, sems.at[0]),
        pltpu.make_async_copy(assign_hbm, assign, sems.at[1]),
        pltpu.make_async_copy(left_hbm, left, sems.at[2]),
        pltpu.make_async_copy(right_hbm, right, sems.at[3]),
    ]
    for copy in copies:
        copy.start()
    for dest in range(8):
        out[dest, pl.ds(8 * W + 4, 4), :] = jnp.zeros((4, 2 * W), F32)
    for copy in copies:
        copy.wait()
    for t in range(4):
        row = jnp.full((1, 2 * W), assign[0, t].astype(F32), F32)
        for dest in range(8):
            out[dest, pl.ds(8 * W + t, 1), :] = row
    for half in range(2):
        for k in range(4):
            kind = layout[0, (1 - half) * NR + 4 * core + k]
            for n, table in ((2 * k, left), (2 * k + 1, right)):
                x = table[0, kind].astype(F32)
                for dest in range(half, 8, 2):
                    out[dest, pl.ds(W * n, W), :] = x


def unpack_column(source, j, part, lefts, rights, sign):
    for k in range(4):
        row = 4 * part + k
        lefts[j, row] = source[j, pl.ds(2 * W * k, W), :].astype(BF16)
        r = source[j, pl.ds(2 * W * k + W, W), :]
        rights[j, row, pl.ds(0, W), :] = r.astype(BF16)
        rights[j, row, pl.ds(W, W), :] = times_i(r, sign).astype(BF16)


def unpack_kernel(mine, cosine, sine, lefts, rights, phases):
    _, _, own, _ = places()
    part, sign = lax.axis_index("c"), sign_row()

    def place(j, unused):
        unpack_column(mine, j, part, lefts, rights, sign)
        return unused

    lax.fori_loop(0, NC, place, 0)
    for j in range(NC):
        value = mine[j, pl.ds(8 * W + own, 1), :]
        for n, table in ((0, cosine), (NC, sine)):
            row = jnp.zeros((1, 2 * W), F32)
            for v in range(4):
                row = jnp.where(value == float(v), table[pl.ds(v, 1), :], row)
            phases[pl.ds(n + j, 1), :] = row


def halves(x):
    high = x.astype(BF16)
    return high, (x - high.astype(F32)).astype(BF16)


def sweep(state, turned, lefts, rights, phases, halo_in, halo_out, peaks, start, sign, prepare=None, entry=None, skip=0):
    def column(j, carry):
        p, rho_mix, rho = carry
        scale = 1.0 / p
        cos_row = phases[pl.ds(j, 1), :] * scale
        sin_row = phases[pl.ds(NC + j, 1), :] * scale
        cos_turn = cos_row * sign
        sin_turn = sin_row * sign
        boards = [state[k] for k in range(NR)]
        turns = [turned[k] for k in range(NR)]
        if j >= skip:
            halo_out[pl.ds((j - skip) * W, W), :] = boards[0]
        if halo_in is None:
            below = below_turn = None
        else:
            if entry is None:
                below = halo_in[pl.ds(j * W, W), :]
            else:
                below = entry if j == 0 else halo_in[pl.ds((j - 1) * W, W), :]
            below = below * (rho_mix * 0.5**NR)
            below_turn = times_i(below, sign)
        top = jnp.zeros((8, 2 * W), F32)
        for k in range(NR):
            after = boards[k + 1] if k + 1 < NR else below
            mixed = boards[k] if after is None else boards[k] + after
            after = turns[k + 1] if k + 1 < NR else below_turn
            turn = turns[k] if after is None else turns[k] + after
            mh, ml = halves(mixed)
            th, tl = halves(turn)
            both = jnp.dot(
                lefts[j, k],
                jnp.concatenate([jnp.concatenate([mh, th], 0), jnp.concatenate([ml, tl], 0)], 1),
                preferred_element_type=F32,
            )
            middle = both[:, : 2 * W] + both[:, 2 * W :]
            dh, dl = halves(middle)
            two = jnp.dot(
                jnp.concatenate([dh, dl], 0), rights[j, k], preferred_element_type=F32
            )
            plain = two[:W] + two[W:]
            flip = pltpu.roll(plain, W, 1)
            out = plain * cos_row + flip * sin_row
            state[k] = out
            turned[k] = flip * cos_turn - plain * sin_turn
            row_top = jnp.abs(out[0:8])
            for g in range(1, 8):
                row_top = jnp.maximum(row_top, jnp.abs(out[8 * g : 8 * g + 8]))
            top = jnp.maximum(top, row_top * 2.0**k)
        own_top = jnp.broadcast_to(jnp.max(top, keepdims=True), (1, 2 * W))
        halo_out[pl.ds((NC - skip) * W + j, 1), :] = own_top
        if halo_in is None:
            other_top = jnp.zeros((1, 2 * W), F32)
        else:
            rows_in = NC if entry is None else NC - 1
            other_top = halo_in[pl.ds(rows_in * W + j, 1), :]
        p_new = jnp.maximum(jnp.maximum(own_top, other_top * rho), 1.0)
        peaks[pl.ds(j, 1), :] = p_new
        return (p_new, rho, rho * jnp.maximum(other_top, 1.0) / p_new)

    carry = start
    if prepare is not None:
        prepare(0)
    for j in range(NC):
        if prepare is not None and j + 1 < NC:
            prepare(j + 1)
        carry = column(j, carry)
    return carry


def close_sums(state, close, base, sign):
    real = jnp.zeros((8, 2 * W), F32)
    imag = jnp.zeros((8, 2 * W), F32)
    for k in range(NR):
        c = close[base + k]
        b = state[k]
        d = pltpu.roll(c, W, 1)
        row_real = b[0:8] * c[0:8]
        row_imag = b[0:8] * d[0:8]
        for g in range(1, 8):
            part = slice(8 * g, 8 * g + 8)
            row_real = row_real + b[part] * c[part]
            row_imag = row_imag + b[part] * d[part]
        real = real + row_real * 2.0**k
        imag = imag + row_imag * 2.0**k
    return -real * sign, imag


def write_messages(state, board_out, halo_out, peaks, ell, end, sums):
    p, rho_mix, rho = end
    for k in range(NR):
        board_out[pl.ds(k * W, W), :] = state[k]
    board_out[pl.ds(NR * W, 1), :] = p
    board_out[pl.ds(NR * W + 1, 1), :] = rho_mix
    board_out[pl.ds(NR * W + 2, 1), :] = rho
    board_out[pl.ds(NR * W + 3, 1), :] = ell + jnp.sum(jnp.log(peaks[...]), axis=0, keepdims=True)
    board_out[pl.ds(NR * W + 4, 4), :] = jnp.zeros((4, 2 * W), F32)
    if sums is not None:
        halo_out[pl.ds(NC * W + 8, 8), :] = sums[0]
        halo_out[pl.ds(NC * W + 16, 8), :] = sums[1]


def places():
    s, q = lax.axis_index("s"), lax.axis_index("q")
    i = jnp.where(s == 0, lax.axis_index("xp"), 1 - lax.axis_index("xp"))
    stays = jnp.logical_or(q == 0, lax.axis_index("c") == 1)
    j = jnp.where(stays, lax.axis_index("yh"), 1 - lax.axis_index("yh"))
    return s, q, 2 * i + j, (1 - q) * NR


def first_kernel(other, lefts_in, rights_in, phases, edge, lefts, rights, board_out, halo_out, state, turned, peaks):
    s, q, _, base = places()
    sign = sign_row()
    one = jnp.ones((1, 2 * W), F32)
    part = 1 - lax.axis_index("c")
    mine = jnp.logical_and(s == 0, q == 0)
    prepare = lambda j: unpack_column(other, j, part, lefts, rights, sign)

    @pl.when(mine)
    def run():
        for k in range(NR):
            x = edge[base + k].astype(F32) * 0.5**k
            state[k] = x
            turned[k] = times_i(x, sign)
        end = sweep(
            state, turned, lefts, rights, phases, None, halo_out, peaks, (one, one, one), sign, prepare, None, 1
        )
        write_messages(state, board_out, halo_out, peaks, 0.0 * one, end, None)

    @pl.when(jnp.logical_not(mine))
    def keep():
        def place(j, unused):
            prepare(j)
            return unused

        lax.fori_loop(0, NC, place, 0)


def load_state(state, turned, edge, board_in, base, s, sign):
    one = jnp.ones((1, 2 * W), F32)
    first = s == 0
    for k in range(NR):
        x = jnp.where(first, edge[base + k].astype(F32) * 0.5**k, board_in[pl.ds(k * W, W), :])
        state[k] = x
        turned[k] = times_i(x, sign)
    row = lambda n: board_in[pl.ds(NR * W + n, 1), :]
    p = jnp.maximum(jnp.where(first, one, row(0)), 1.0)
    rho_mix = jnp.where(first, one, row(1))
    rho = jnp.where(first, one, row(2))
    ell = jnp.where(first, 0.0 * one, row(3))
    return (p, rho_mix, rho), ell


def second_kernel(phases, edge, lefts, rights, close, board_in, halo_in, board_out, halo_out, state, turned, peaks):
    s, q, _, base = places()

    @pl.when(s != q)
    def run():
        sign = sign_row()
        start, ell = load_state(state, turned, edge, board_in, base, s, sign)
        entry = jnp.where(s == 0, edge[NR].astype(F32), 0.0)
        end = sweep(
            state, turned, lefts, rights, phases, halo_in, halo_out, peaks, start, sign, None, entry
        )
        sums = close_sums(state, close, base, sign)
        write_messages(state, board_out, halo_out, peaks, ell, end, sums)


def third_kernel(phases, edge, lefts, rights, close, board_in, halo_in, out, state, turned, peaks, halo_out):
    s, q, own, base = places()
    mine = jnp.logical_and(s == 1, q == 1)

    @pl.when(mine)
    def run():
        sign = sign_row()
        start, ell = load_state(state, turned, edge, board_in, base, s, sign)
        p, rho_mix, _ = sweep(
            state, turned, lefts, rights, phases, halo_in, halo_out, peaks, start, sign
        )
        ell = ell + jnp.sum(jnp.log(peaks[...]), axis=0, keepdims=True)
        real, imag = close_sums(state, close, base, sign)
        factor = 1.0 / math.sqrt(2 * NR * W * W)
        scale = factor / p
        real = real + rho_mix * halo_in[pl.ds(NC * W + 8, 8), :]
        imag = imag + rho_mix * halo_in[pl.ds(NC * W + 16, 8), :]
        real = jnp.sum(real, keepdims=True) * scale
        imag = jnp.sum(imag, keepdims=True) * scale
        index = 4 * (2 * lax.axis_index("z") + lax.axis_index("c")) + own
        lane = lax.broadcasted_iota(jnp.int32, (1, 2 * W), 1)
        row = jnp.where(lane == index, real, 0.0)
        row = row + jnp.where(lane == index + 32, imag, 0.0)
        row = row + jnp.where(lane == index + 64, ell, 0.0)
        out[...] = row

    @pl.when(jnp.logical_not(mine))
    def nothing():
        out[...] = jnp.zeros((1, 2 * W), F32)


def finish_kernel(blocks, amps, logs, total, top):
    found = jnp.sum(blocks[...], axis=0, keepdims=True)
    real, imag, ell = found, pltpu.roll(found, 96, 1), pltpu.roll(found, 64, 1)
    used = lax.broadcasted_iota(jnp.int32, (1, 2 * W), 1) < 32
    high = jnp.max(jnp.where(used, ell, 0.0), axis=1, keepdims=True)
    weight = jnp.where(used, jnp.exp(jnp.where(used, ell - high, 0.0)), 0.0)
    top[...] = high
    sums = [jnp.sum(x * weight, axis=1, keepdims=True) for x in (real, imag)]
    total[...] = jnp.concatenate(sums, 1)
    at = 4 * (2 * lax.axis_index("z") + lax.axis_index("c"))
    shift = jnp.where(at == 0, 0, 2 * W - at)
    amps[0:1, :] = pltpu.roll(real, shift, 1)[:, 0:4]
    amps[1:2, :] = pltpu.roll(imag, shift, 1)[:, 0:4]
    logs[...] = pltpu.roll(ell, shift, 1)[:, 0:4]


def call(kernel, outs, scratch, args, specs=None, aliases=None):
    return pl.pallas_call(
        kernel,
        out_shape=outs,
        in_specs=specs or [vmem()] * len(args),
        out_specs=jax.tree.map(lambda _: vmem(), outs),
        scratch_shapes=scratch,
        input_output_aliases=aliases or {},
        compiler_params=pltpu.CompilerParams(vmem_limit_bytes=20 * 2**20),
    )(*args)


def shape(*dims, dtype=F32):
    return jax.ShapeDtypeStruct(dims, dtype)


def chip(s, xp, yh, q):
    return 8 * s + 4 * xp + 2 * yh + q


def along_columns(value, q):
    pairs = [(chip(0, xp, yh, q), chip(1, 1 - xp, yh, q)) for xp in range(2) for yh in range(2)]
    return lax.ppermute(value, GRID, pairs)


def along_rows(value, s):
    pairs = []
    for xp in range(2):
        for yh in range(2):
            source = 2 * chip(s, xp, yh, 0)
            pairs.append((source, 2 * chip(s, xp, 1 - yh, 1)))
            pairs.append((source + 1, 2 * chip(s, xp, yh, 1) + 1))
    return lax.ppermute(value, (*GRID, "c"), pairs)


def swapped(value):
    return lax.ppermute(value, "c", [(0, 1), (1, 0)])


def gathered(found):
    count = lax.axis_size(AXES)
    spread = jnp.broadcast_to(found[None], (count, *found.shape))
    return lax.all_to_all(spread, AXES, 0, 0, tiled=True).reshape(count, found.shape[1])


def body(layout, assign, edge, gate_left, gate_right, phase_angle, close):
    cosine, sine = jnp.cos(phase_angle), jnp.sin(phase_angle)
    cosine = jnp.concatenate([cosine, cosine], -1)
    sine = jnp.concatenate([-sine, sine], -1)
    hbm = pl.BlockSpec(memory_space=pltpu.HBM)
    packed = call(
        pack_kernel,
        shape(8, BLOCK, 2 * W),
        [
            pltpu.SMEM((1, 16), jnp.int32),
            pltpu.SMEM((1, 4), jnp.int32),
            pltpu.VMEM(gate_left.shape, BF16),
            pltpu.VMEM(gate_right.shape, BF16),
            pltpu.SemaphoreType.DMA((4,)),
        ],
        [
            pltpu.with_memory_space_constraint(x, pltpu.HBM)
            for x in (layout.T, assign.T, gate_left, gate_right)
        ],
        [hbm, hbm, hbm, hbm],
    )
    mine = lax.all_to_all(packed, ("xp", "yh", "q"), 0, 0, tiled=True)
    other = swapped(mine)
    state = pltpu.VMEM((NR, W, 2 * W), F32)
    peaks = pltpu.VMEM((NC, 2 * W), F32)
    gates = (shape(NC, NR, W, 2 * W, dtype=BF16), shape(NC, NR, 2 * W, 2 * W, dtype=BF16))
    lefts, rights, phases = call(
        unpack_kernel, (*gates, shape(2 * NC, 2 * W)), [], (mine, cosine, sine)
    )
    lefts, rights, board, halo = call(
        first_kernel,
        (*gates, shape(BOARD, 2 * W), shape(FIRST, 2 * W)),
        [state, state, peaks],
        (other, lefts, rights, phases, edge),
        aliases={1: 0, 2: 1},
    )
    board = along_columns(board, 0)
    halo = along_rows(halo, 0)
    board, halo = call(
        second_kernel,
        (shape(BOARD, 2 * W), shape(HALO, 2 * W)),
        [state, state, peaks],
        (phases, edge, lefts, rights, close, board, halo),
    )
    board, halo = along_columns(board, 1), along_rows(halo, 1)
    found = call(
        third_kernel,
        shape(1, 2 * W),
        [state, state, peaks, pltpu.VMEM((HALO, 2 * W), F32)],
        (phases, edge, lefts, rights, close, board, halo),
    )
    amps, logs, total_amp, top_log = call(
        finish_kernel,
        (shape(2, 4), shape(1, 4), shape(1, 2), shape(1, 1)),
        [],
        (gathered(found),),
    )
    return (amps.T, logs.reshape(4), total_amp.reshape(2), top_log.reshape(()))


def solution(mesh):
    split = Mesh(mesh.devices.reshape(2, 2, 2, 2, 4, 2), AXES)
    placed = (
        P(None, GRID),
        P(("z", "c"), GRID),
        P(),
        P(GRID, None, None, None),
        P(GRID, None, None, None),
        P(),
        P(),
    )
    return jax.shard_map(
        body,
        mesh=split,
        in_specs=placed,
        out_specs=(P(("z", "c"), None), P(("z", "c")), P(), P()),
        check_vma=False,
    )
```

```python
import math

import jax
import jax.numpy as jnp
from jax import lax
from jax.experimental import pallas as pl
from jax.experimental.pallas import tpu as pltpu
from jax.sharding import Mesh
from jax.sharding import PartitionSpec as P

AXES = ("s", "xp", "yh", "q", "z", "c")
GRID = ("s", "xp", "yh", "q")
NC = 8
NR = 8
W = 64
BLOCK = 4 * 2 * W + 8
BOARD = NR * W + 8
HALO = NC * W + 24
FIRST = (NC - 1) * W + 8
F32 = jnp.float32
BF16 = jnp.bfloat16


def vmem():
    return pl.BlockSpec(memory_space=pltpu.VMEM)


def sign_row():
    lane = lax.broadcasted_iota(jnp.int32, (1, 2 * W), 1)
    return jnp.where(lane < W, -1.0, 1.0).astype(F32)


def times_i(x, sign):
    return pltpu.roll(x, W, 1) * sign


def pack_kernel(layout_hbm, assign_hbm, left_hbm, right_hbm, out, layout, assign, left, right, sems):
    core = lax.axis_index("c")
    copies = [
        pltpu.make_async_copy(layout_hbm, layout, sems.at[0]),
        pltpu.make_async_copy(assign_hbm, assign, sems.at[1]),
        pltpu.make_async_copy(left_hbm, left, sems.at[2]),
        pltpu.make_async_copy(right_hbm, right, sems.at[3]),
    ]
    for copy in copies:
        copy.start()
    for dest in range(8):
        out[dest, pl.ds(8 * W + 4, 4), :] = jnp.zeros((4, 2 * W), F32)
    for copy in copies:
        copy.wait()
    for t in range(4):
        row = jnp.full((1, 2 * W), assign[0, t].astype(F32), F32)
        for dest in range(8):
            out[dest, pl.ds(8 * W + t, 1), :] = row
    for half in range(2):
        for k in range(4):
            kind = layout[0, (1 - half) * NR + 4 * core + k]
            for n, table in ((2 * k, left), (2 * k + 1, right)):
                x = table[0, kind].astype(F32)
                for dest in range(half, 8, 2):
                    out[dest, pl.ds(W * n, W), :] = x


def unpack_column(source, j, part, lefts, rights, sign):
    for k in range(4):
        row = 4 * part + k
        lefts[j, row] = source[j, pl.ds(2 * W * k, W), :].astype(BF16)
        r = source[j, pl.ds(2 * W * k + W, W), :]
        rights[j, row, pl.ds(0, W), :] = r.astype(BF16)
        rights[j, row, pl.ds(W, W), :] = times_i(r, sign).astype(BF16)


def unpack_kernel(mine, cosine, sine, lefts, rights, phases):
    _, _, own, _ = places()
    part, sign = lax.axis_index("c"), sign_row()

    def place(j, unused):
        unpack_column(mine, j, part, lefts, rights, sign)
        return unused

    lax.fori_loop(0, NC, place, 0)
    for j in range(NC):
        value = mine[j, pl.ds(8 * W + own, 1), :]
        for n, table in ((0, cosine), (NC, sine)):
            row = jnp.zeros((1, 2 * W), F32)
            for v in range(4):
                row = jnp.where(value == float(v), table[pl.ds(v, 1), :], row)
            phases[pl.ds(n + j, 1), :] = row


def halves(x):
    high = x.astype(BF16)
    return high, (x - high.astype(F32)).astype(BF16)


def sweep(state, turned, lefts, rights, phases, halo_in, halo_out, peaks, start, sign, prepare=None, entry=None, skip=0):
    def column(j, carry):
        p, rho_mix, rho = carry
        scale = 1.0 / p
        cos_row = phases[pl.ds(j, 1), :] * scale
        sin_row = phases[pl.ds(NC + j, 1), :] * scale
        cos_turn = cos_row * sign
        sin_turn = sin_row * sign
        boards = [state[k] for k in range(NR)]
        turns = [turned[k] for k in range(NR)]
        if j >= skip:
            halo_out[pl.ds((j - skip) * W, W), :] = boards[0]
        if halo_in is None:
            below = below_turn = None
        else:
            if entry is None:
                below = halo_in[pl.ds(j * W, W), :]
            else:
                below = entry if j == 0 else halo_in[pl.ds((j - 1) * W, W), :]
            below = below * (rho_mix * 0.5**NR)
            below_turn = times_i(below, sign)
        top = jnp.zeros((8, 2 * W), F32)
        for k in range(NR):
            after = boards[k + 1] if k + 1 < NR else below
            mixed = boards[k] if after is None else boards[k] + after
            after = turns[k + 1] if k + 1 < NR else below_turn
            turn = turns[k] if after is None else turns[k] + after
            mh, ml = halves(mixed)
            th, tl = halves(turn)
            both = jnp.dot(
                lefts[j, k],
                jnp.concatenate([jnp.concatenate([mh, th], 0), jnp.concatenate([ml, tl], 0)], 1),
                preferred_element_type=F32,
            )
            middle = both[:, : 2 * W] + both[:, 2 * W :]
            dh, dl = halves(middle)
            right = rights[j, k]
            plain = jnp.dot(
                jnp.concatenate([dh, dl], 1),
                jnp.concatenate([right, right], 0),
                preferred_element_type=F32,
            )
            flip = pltpu.roll(plain, W, 1)
            out = plain * cos_row + flip * sin_row
            state[k] = out
            turned[k] = flip * cos_turn - plain * sin_turn
            row_top = jnp.abs(out[0:8])
            for g in range(1, 8):
                row_top = jnp.maximum(row_top, jnp.abs(out[8 * g : 8 * g + 8]))
            top = jnp.maximum(top, row_top * 2.0**k)
        own_top = jnp.broadcast_to(jnp.max(top, keepdims=True), (1, 2 * W))
        halo_out[pl.ds((NC - skip) * W + j, 1), :] = own_top
        if halo_in is None:
            other_top = jnp.zeros((1, 2 * W), F32)
        else:
            rows_in = NC if entry is None else NC - 1
            other_top = halo_in[pl.ds(rows_in * W + j, 1), :]
        p_new = jnp.maximum(jnp.maximum(own_top, other_top * rho), 1.0)
        peaks[pl.ds(j, 1), :] = p_new
        return (p_new, rho, rho * jnp.maximum(other_top, 1.0) / p_new)

    carry = start
    if prepare is not None:
        prepare(0)
    for j in range(NC):
        if prepare is not None and j + 1 < NC:
            prepare(j + 1)
        carry = column(j, carry)
    return carry


def close_sums(state, close, base, sign):
    real = jnp.zeros((8, 2 * W), F32)
    imag = jnp.zeros((8, 2 * W), F32)
    for k in range(NR):
        c = close[base + k]
        b = state[k]
        d = pltpu.roll(c, W, 1)
        row_real = b[0:8] * c[0:8]
        row_imag = b[0:8] * d[0:8]
        for g in range(1, 8):
            part = slice(8 * g, 8 * g + 8)
            row_real = row_real + b[part] * c[part]
            row_imag = row_imag + b[part] * d[part]
        real = real + row_real * 2.0**k
        imag = imag + row_imag * 2.0**k
    return -real * sign, imag


def write_messages(state, board_out, halo_out, peaks, ell, end, sums):
    p, rho_mix, rho = end
    for k in range(NR):
        board_out[pl.ds(k * W, W), :] = state[k]
    board_out[pl.ds(NR * W, 1), :] = p
    board_out[pl.ds(NR * W + 1, 1), :] = rho_mix
    board_out[pl.ds(NR * W + 2, 1), :] = rho
    board_out[pl.ds(NR * W + 3, 1), :] = ell + jnp.sum(jnp.log(peaks[...]), axis=0, keepdims=True)
    board_out[pl.ds(NR * W + 4, 4), :] = jnp.zeros((4, 2 * W), F32)
    if sums is not None:
        halo_out[pl.ds(NC * W + 8, 8), :] = sums[0]
        halo_out[pl.ds(NC * W + 16, 8), :] = sums[1]


def places():
    s, q = lax.axis_index("s"), lax.axis_index("q")
    i = jnp.where(s == 0, lax.axis_index("xp"), 1 - lax.axis_index("xp"))
    stays = jnp.logical_or(q == 0, lax.axis_index("c") == 1)
    j = jnp.where(stays, lax.axis_index("yh"), 1 - lax.axis_index("yh"))
    return s, q, 2 * i + j, (1 - q) * NR


def first_kernel(other, lefts_in, rights_in, phases, edge, lefts, rights, board_out, halo_out, state, turned, peaks):
    s, q, _, base = places()
    sign = sign_row()
    one = jnp.ones((1, 2 * W), F32)
    part = 1 - lax.axis_index("c")
    mine = jnp.logical_and(s == 0, q == 0)
    prepare = lambda j: unpack_column(other, j, part, lefts, rights, sign)

    @pl.when(mine)
    def run():
        for k in range(NR):
            x = edge[base + k].astype(F32) * 0.5**k
            state[k] = x
            turned[k] = times_i(x, sign)
        end = sweep(
            state, turned, lefts, rights, phases, None, halo_out, peaks, (one, one, one), sign, prepare, None, 1
        )
        write_messages(state, board_out, halo_out, peaks, 0.0 * one, end, None)

    @pl.when(jnp.logical_not(mine))
    def keep():
        def place(j, unused):
            prepare(j)
            return unused

        lax.fori_loop(0, NC, place, 0)


def load_state(state, turned, edge, board_in, base, s, sign):
    one = jnp.ones((1, 2 * W), F32)
    first = s == 0
    for k in range(NR):
        x = jnp.where(first, edge[base + k].astype(F32) * 0.5**k, board_in[pl.ds(k * W, W), :])
        state[k] = x
        turned[k] = times_i(x, sign)
    row = lambda n: board_in[pl.ds(NR * W + n, 1), :]
    p = jnp.maximum(jnp.where(first, one, row(0)), 1.0)
    rho_mix = jnp.where(first, one, row(1))
    rho = jnp.where(first, one, row(2))
    ell = jnp.where(first, 0.0 * one, row(3))
    return (p, rho_mix, rho), ell


def second_kernel(phases, edge, lefts, rights, close, board_in, halo_in, board_out, halo_out, state, turned, peaks):
    s, q, _, base = places()

    @pl.when(s != q)
    def run():
        sign = sign_row()
        start, ell = load_state(state, turned, edge, board_in, base, s, sign)
        entry = jnp.where(s == 0, edge[NR].astype(F32), 0.0)
        end = sweep(
            state, turned, lefts, rights, phases, halo_in, halo_out, peaks, start, sign, None, entry
        )
        sums = close_sums(state, close, base, sign)
        write_messages(state, board_out, halo_out, peaks, ell, end, sums)


def third_kernel(phases, edge, lefts, rights, close, board_in, halo_in, out, state, turned, peaks, halo_out):
    s, q, own, base = places()
    mine = jnp.logical_and(s == 1, q == 1)

    @pl.when(mine)
    def run():
        sign = sign_row()
        start, ell = load_state(state, turned, edge, board_in, base, s, sign)
        p, rho_mix, _ = sweep(
            state, turned, lefts, rights, phases, halo_in, halo_out, peaks, start, sign
        )
        ell = ell + jnp.sum(jnp.log(peaks[...]), axis=0, keepdims=True)
        real, imag = close_sums(state, close, base, sign)
        factor = 1.0 / math.sqrt(2 * NR * W * W)
        scale = factor / p
        real = real + rho_mix * halo_in[pl.ds(NC * W + 8, 8), :]
        imag = imag + rho_mix * halo_in[pl.ds(NC * W + 16, 8), :]
        real = jnp.sum(real, keepdims=True) * scale
        imag = jnp.sum(imag, keepdims=True) * scale
        index = 4 * (2 * lax.axis_index("z") + lax.axis_index("c")) + own
        lane = lax.broadcasted_iota(jnp.int32, (1, 2 * W), 1)
        row = jnp.where(lane == index, real, 0.0)
        row = row + jnp.where(lane == index + 32, imag, 0.0)
        row = row + jnp.where(lane == index + 64, ell, 0.0)
        out[...] = row

    @pl.when(jnp.logical_not(mine))
    def nothing():
        out[...] = jnp.zeros((1, 2 * W), F32)


def finish_kernel(blocks, amps, logs, total, top):
    found = jnp.sum(blocks[...], axis=0, keepdims=True)
    real, imag, ell = found, pltpu.roll(found, 96, 1), pltpu.roll(found, 64, 1)
    used = lax.broadcasted_iota(jnp.int32, (1, 2 * W), 1) < 32
    high = jnp.max(jnp.where(used, ell, 0.0), axis=1, keepdims=True)
    weight = jnp.where(used, jnp.exp(jnp.where(used, ell - high, 0.0)), 0.0)
    top[...] = high
    sums = [jnp.sum(x * weight, axis=1, keepdims=True) for x in (real, imag)]
    total[...] = jnp.concatenate(sums, 1)
    at = 4 * (2 * lax.axis_index("z") + lax.axis_index("c"))
    shift = jnp.where(at == 0, 0, 2 * W - at)
    amps[0:1, :] = pltpu.roll(real, shift, 1)[:, 0:4]
    amps[1:2, :] = pltpu.roll(imag, shift, 1)[:, 0:4]
    logs[...] = pltpu.roll(ell, shift, 1)[:, 0:4]


def call(kernel, outs, scratch, args, specs=None, aliases=None):
    return pl.pallas_call(
        kernel,
        out_shape=outs,
        in_specs=specs or [vmem()] * len(args),
        out_specs=jax.tree.map(lambda _: vmem(), outs),
        scratch_shapes=scratch,
        input_output_aliases=aliases or {},
        compiler_params=pltpu.CompilerParams(vmem_limit_bytes=20 * 2**20),
    )(*args)


def shape(*dims, dtype=F32):
    return jax.ShapeDtypeStruct(dims, dtype)


def chip(s, xp, yh, q):
    return 8 * s + 4 * xp + 2 * yh + q


def along_columns(value, q):
    pairs = [(chip(0, xp, yh, q), chip(1, 1 - xp, yh, q)) for xp in range(2) for yh in range(2)]
    return lax.ppermute(value, GRID, pairs)


def along_rows(value, s):
    pairs = []
    for xp in range(2):
        for yh in range(2):
            source = 2 * chip(s, xp, yh, 0)
            pairs.append((source, 2 * chip(s, xp, 1 - yh, 1)))
            pairs.append((source + 1, 2 * chip(s, xp, yh, 1) + 1))
    return lax.ppermute(value, (*GRID, "c"), pairs)


def swapped(value):
    return lax.ppermute(value, "c", [(0, 1), (1, 0)])


def gathered(found):
    count = lax.axis_size(AXES)
    spread = jnp.broadcast_to(found[None], (count, *found.shape))
    return lax.all_to_all(spread, AXES, 0, 0, tiled=True).reshape(count, found.shape[1])


def body(layout, assign, edge, gate_left, gate_right, phase_angle, close):
    cosine, sine = jnp.cos(phase_angle), jnp.sin(phase_angle)
    cosine = jnp.concatenate([cosine, cosine], -1)
    sine = jnp.concatenate([-sine, sine], -1)
    hbm = pl.BlockSpec(memory_space=pltpu.HBM)
    packed = call(
        pack_kernel,
        shape(8, BLOCK, 2 * W),
        [
            pltpu.SMEM((1, 16), jnp.int32),
            pltpu.SMEM((1, 4), jnp.int32),
            pltpu.VMEM(gate_left.shape, BF16),
            pltpu.VMEM(gate_right.shape, BF16),
            pltpu.SemaphoreType.DMA((4,)),
        ],
        [
            pltpu.with_memory_space_constraint(x, pltpu.HBM)
            for x in (layout.T, assign.T, gate_left, gate_right)
        ],
        [hbm, hbm, hbm, hbm],
    )
    mine = lax.all_to_all(packed, ("xp", "yh", "q"), 0, 0, tiled=True)
    other = swapped(mine)
    state = pltpu.VMEM((NR, W, 2 * W), F32)
    peaks = pltpu.VMEM((NC, 2 * W), F32)
    gates = (shape(NC, NR, W, 2 * W, dtype=BF16), shape(NC, NR, 2 * W, 2 * W, dtype=BF16))
    lefts, rights, phases = call(
        unpack_kernel, (*gates, shape(2 * NC, 2 * W)), [], (mine, cosine, sine)
    )
    lefts, rights, board, halo = call(
        first_kernel,
        (*gates, shape(BOARD, 2 * W), shape(FIRST, 2 * W)),
        [state, state, peaks],
        (other, lefts, rights, phases, edge),
        aliases={1: 0, 2: 1},
    )
    board = along_columns(board, 0)
    halo = along_rows(halo, 0)
    board, halo = call(
        second_kernel,
        (shape(BOARD, 2 * W), shape(HALO, 2 * W)),
        [state, state, peaks],
        (phases, edge, lefts, rights, close, board, halo),
    )
    board, halo = along_columns(board, 1), along_rows(halo, 1)
    found = call(
        third_kernel,
        shape(1, 2 * W),
        [state, state, peaks, pltpu.VMEM((HALO, 2 * W), F32)],
        (phases, edge, lefts, rights, close, board, halo),
    )
    amps, logs, total_amp, top_log = call(
        finish_kernel,
        (shape(2, 4), shape(1, 4), shape(1, 2), shape(1, 1)),
        [],
        (gathered(found),),
    )
    return (amps.T, logs.reshape(4), total_amp.reshape(2), top_log.reshape(()))


def solution(mesh):
    split = Mesh(mesh.devices.reshape(2, 2, 2, 2, 4, 2), AXES)
    placed = (
        P(None, GRID),
        P(("z", "c"), GRID),
        P(),
        P(GRID, None, None, None),
        P(GRID, None, None, None),
        P(),
        P(),
    )
    return jax.shard_map(
        body,
        mesh=split,
        in_specs=placed,
        out_specs=(P(("z", "c"), None), P(("z", "c")), P(), P()),
        check_vma=False,
    )
```
